32 devices in a mesh: chain: 4 (over x, core), depth: 8 (over z, y).
Axes of the slice: x: 2, y: 2, z: 4, core: 2. Of those that a mesh axis runs over, the one named last changes fastest.
Arguments:
- model_field: float32 [256, 2048], P(('chain', 'depth')), parts along dimension 0, may hold values from -4 to 4
- column_rate: float32 [8192], P('chain'), parts along dimension 0, may hold values from 0.2 to 20
- wavelets: float32 [64, 2048], P('chain'), parts along dimension 0, may hold values from -6 to 6
- source_depth: int32 [64], P('chain'), parts along dimension 0, may hold values from 0 to 63
- observed: float32 [256, 16, 2048], P(('chain', 'depth')), parts along dimension 0, may hold values from -3 to 3
- basis: bfloat16 [1024, 64, 2048], P('chain', 'depth'), parts along dimension 0, may hold values from -0.0625 to 0.0625
- curvature: float32 [1024], P('chain'), parts along dimension 0, may hold values from 0.5 to 50
- noise_draw: float32 [256, 2048], P(('chain', 'depth')), parts along dimension 0, may hold values from -6 to 6
Outputs:
- proposal: float32 [256, 2048], P(('chain', 'depth')), parts along dimension 0
- log_gain: float32 [4], P('chain'), parts along dimension 0
The draws below stay inside these ranges and needn't reach their ends.
There are 4 independent parts, one for each index of `chain`. The reference program is written for one: setup_inputs(seed, part) draws one part's arguments, and reference() takes and returns one part's arrays. A program takes and returns all parts, laid end to end along the dimension named above; each array names one. Nothing has to cross between parts.
All inputs are finite; a program needn't handle non-finite values.
Results may differ from the reference program's by a relative error of at most 0.0003.
The reference program's roundings to bfloat16 on the way count: a program that leaves them out, or rounds other values in their place, can miss the bound.
Values sent between devices are 32-bit elements; how exact they have to be, the bound alone decides.
No kernel may reach another device: no remote copies, remote signals or barrier semaphores. Data moves between devices by JAX's collectives and lax.ppermute only.
A program may use at most 64 MiB of HBM per device.

```python
import math
import jax
import jax.numpy as jnp
from jax import lax

LAT = 2048
NSRC = 16
RANK = 256
NZ = 64


def with_ends(array, stream_key, low, largest):
    place = [jax.random.randint(jax.random.fold_in(stream_key, axis), (), 0, length) for axis, length in enumerate(array.shape)]
    longest = array.shape.index(max(array.shape))
    neighbour = place[:longest] + [(place[longest] + 1) % array.shape[longest]] + place[longest + 1:]
    return array.at[tuple(place)].set(low).at[tuple(neighbour)].set(largest)


def block_levels(own_key, shape, cuts, least, largest):
    factor_of, own = 1.0, jax.random.fold_in(own_key, 6)
    for dim, parts in cuts:
        heights = jnp.exp(jax.random.uniform(jax.random.fold_in(own, dim), (parts,), jnp.float32, least / len(cuts), largest / len(cuts)))
        factor_of = factor_of * jnp.repeat(heights, shape[dim] // parts).reshape([-1 if axis == dim else 1 for axis in range(len(shape))])
    return factor_of


def noise(own_key, dims, spread, limit, shards=(), kind=jnp.bfloat16):
    gain = block_levels(own_key, dims, shards, -0.22, 0.18) if shards else 1.0
    drawn = jax.random.normal(own_key, dims, jnp.float32) * spread * gain
    return jnp.minimum(jnp.maximum(drawn, -limit), limit).astype(kind)


def setup_inputs(seed: int = 0, part: int = 0) -> dict:
    arg_keys = jax.random.split(jax.random.key(seed), 9)
    own_keys = jax.random.split(jax.random.fold_in(arg_keys[8], part), 9)
    return {
        "model_field": noise(own_keys[0], (NZ, LAT), 1.0, 4.0, ((0, 8),), jnp.float32),
        "column_rate": jnp.clip(jnp.exp(jax.random.uniform(own_keys[1], (LAT,), jnp.float32, math.log(0.2), math.log(20.0))), 0.2, 20.0),
        "wavelets": noise(own_keys[2], (NSRC, LAT), 1.0, 6.0, (), jnp.float32),
        "source_depth": with_ends(jax.random.randint(own_keys[3], (NSRC,), 0, NZ), jax.random.fold_in(own_keys[3], 1), 0, NZ - 1).astype(jnp.int32),
        "observed": noise(own_keys[4], (NZ, NSRC, LAT), 0.5, 3.0, ((0, 8),), jnp.float32),
        "basis": noise(own_keys[5], (RANK, NZ, LAT), (NZ * LAT // 16) ** -0.5, 0.0625, ((1, 8),)),
        "curvature": jnp.clip(jnp.exp(jax.random.uniform(own_keys[6], (RANK,), jnp.float32, math.log(0.5), math.log(50.0))), 0.5, 50.0),
        "noise_draw": noise(own_keys[7], (NZ, LAT), 1.0, 6.0, ((0, 8),), jnp.float32),
    }


def coefficients(model, column_rate, depth_count):
    coef = (column_rate / depth_count)[None, :] * jnp.exp(0.5 * model)
    return (coef, jnp.exp(-coef))

def march_down(decay, wavelets, source_depth):
    layers = jnp.arange(decay.shape[0], dtype=jnp.int32)

    def advance(state, inputs):
        factor, layer = inputs
        inject = jnp.where((source_depth == layer)[:, None], wavelets, jnp.zeros_like(wavelets))
        state = factor[None, :] * state + inject
        return (state, state)
    start = jnp.zeros(wavelets.shape, wavelets.dtype)
    _, fields = lax.scan(advance, start, (decay, layers))
    return fields

def march_up(decay, misfit_field):

    def retreat(carry, inputs):
        factor, resid = inputs
        adjoint = resid + carry
        return (factor[None, :] * adjoint, adjoint)
    start = jnp.zeros(misfit_field.shape[1:], misfit_field.dtype)
    _, adjoints = lax.scan(retreat, start, (decay, misfit_field), reverse=True)
    return adjoints

def energy(model, column_rate, wavelets, source_depth, observed):
    coef, decay = coefficients(model, column_rate, model.shape[0])
    fields = march_down(decay, wavelets, source_depth)
    resid = fields - observed
    value = jnp.sum(resid * resid) / wavelets.shape[0] + 0.5 * jnp.sum(model * model)
    return (value, coef, decay, fields, resid)

def reference(model_field, column_rate, wavelets, source_depth, observed, basis, curvature, noise_draw):
    sources = wavelets.shape[0]
    before, coef, decay, fields, resid = energy(model_field, column_rate, wavelets, source_depth, observed)
    adjoints = march_up(decay, resid)
    previous = jnp.concatenate([jnp.zeros_like(fields[:1]), fields[:-1]], axis=0)
    gradient = model_field - coef * decay / sources * lax.optimization_barrier(jnp.sum(adjoints * previous, axis=1))
    flat_basis = basis.reshape(basis.shape[0], -1)
    stacked = jnp.stack([gradient.reshape(-1), noise_draw.reshape(-1)]).astype(jnp.bfloat16)
    projected = lax.dot_general(stacked, flat_basis, (((1,), (1,)), ((), ())), preferred_element_type=jnp.float32)
    damping = curvature / (1.0 + curvature)
    shrink = 1.0 - 1.0 / jnp.sqrt(1.0 + curvature)
    mixed = (damping * projected[0] - shrink * projected[1]).astype(jnp.bfloat16)
    correction = jnp.dot(mixed, flat_basis, preferred_element_type=jnp.float32).reshape(model_field.shape)
    proposal = model_field - gradient + noise_draw + correction
    after = energy(proposal, column_rate, wavelets, source_depth, observed)[0]
    cells = model_field.shape[0] * model_field.shape[1]
    log_gain = jnp.reshape((before - after) / cells, (1,))
    return (proposal, log_gain)
```

```python
import functools

import jax
import jax.numpy as jnp
from jax import lax
from jax.experimental import pallas as pl
from jax.experimental.pallas import tpu as pltpu
from jax.sharding import PartitionSpec as P

LANES = 128
f32 = jnp.float32


def pad_rows(rows):
    return -(-rows // 8) * 8


def source_layers(sd_ref, count, width):
    row = lax.broadcasted_iota(jnp.int32, (count, width), 0)
    layers = jnp.zeros((count, width), jnp.int32)
    for k in range(count):
        layers = jnp.where(row == k, sd_ref[k], layers)
    return layers


def summarize(coef, w, sd, first, obs_ref, lanes):
    nz = coef.shape[0]
    decay = jnp.exp(-coef)
    above = sd < first
    f = jnp.where(above, 1.0, 0.0)
    through = jnp.ones((1, coef.shape[1]), f32)
    squares = jnp.zeros_like(through)
    cross = jnp.zeros_like(w)
    own = jnp.zeros_like(w)
    for z in range(nz):
        step = decay[z : z + 1]
        f = step * f + jnp.where(sd == first + z, w, 0.0)
        through = through * step
        squares = squares + through * through
        cross = cross + f * obs_ref[z, :, lanes]
        own = own + f * f
    rows = jnp.where(above, cross, f)
    part = jnp.where(above, 0.0, own - 2.0 * cross)
    return rows, through, squares, part


def total(x):
    return jnp.sum(jnp.sum(x, axis=0, keepdims=True), axis=1, keepdims=True)


def write_summary(out_ref, n, rows, through, squares):
    k = rows.shape[0]
    out_ref[n, 0:k, :] = rows
    out_ref[n, k : k + 1, :] = through
    out_ref[n, k + 1 : k + 2, :] = squares


def first_kernel(depth_count, sd_ref, model_ref, rate_ref, w_ref, obs_ref, out_ref, energy_ref):
    blocks, width = out_ref.shape[0], out_ref.shape[2]
    nz = model_ref.shape[0]
    sd = source_layers(sd_ref, w_ref.shape[0], width)
    first = lax.axis_index("depth") * nz
    energy = jnp.zeros((1, 1), f32)
    for n in range(blocks):
        lanes = slice(n * width, (n + 1) * width)
        model = model_ref[:, lanes]
        coef = rate_ref[:, lanes] * (1.0 / depth_count) * jnp.exp(0.5 * model)
        rows, through, squares, part = summarize(coef, w_ref[:, lanes], sd, first, obs_ref, lanes)
        write_summary(out_ref, n, rows, through, squares)
        energy = energy + total(part) / w_ref.shape[0] + 0.5 * total(model * model)
    energy_ref[...] = jnp.broadcast_to(energy, energy_ref.shape)


def scan_slabs(sd, nz, got_ref):
    blocks = got_ref.shape[0]
    k = sd.shape[0]
    carry = jnp.zeros(sd.shape, f32)
    energy = jnp.zeros(sd.shape, f32)
    carries = []
    for n in range(blocks):
        rows = got_ref[n, 0:k, :]
        through = got_ref[n, k : k + 1, :]
        squares = got_ref[n, k + 1 : k + 2, :]
        carries.append(carry)
        energy = energy + carry * (carry * squares - 2.0 * rows)
        carry = through * carry + jnp.where(sd >= n * nz, rows, 0.0)
    return carries, energy


def owner_kernel(nz, sd_ref, got_ref, out_ref, energy_ref):
    blocks, _, width = got_ref.shape
    k = sd_ref.shape[0]
    sd = source_layers(sd_ref, k, width)
    carries, energy = scan_slabs(sd, nz, got_ref)
    deeper = jnp.zeros(sd.shape, f32)
    for n in reversed(range(blocks)):
        above = sd < n * nz
        out_ref[n, 0:k, :] = jnp.where(above, carries[n], deeper)
        out_ref[n, k : k + 1, :] = jnp.sum(jnp.where(above, deeper, 0.0), axis=0, keepdims=True)
        rows = got_ref[n, 0:k, :]
        squares = got_ref[n, k + 1 : k + 2, :]
        deeper = deeper + carries[n] * (carries[n] * squares - rows)
    energy_ref[...] = jnp.broadcast_to(total(energy) / k, energy_ref.shape)


def gradient_kernel(
    depth_count, sd_ref, got_ref, model_ref, rate_ref, w_ref, obs_ref, noise_ref, basis_ref,
    gradient_ref, out_ref, sums_ref
):
    blocks, _, width = got_ref.shape
    nz = model_ref.shape[0]
    k = w_ref.shape[0]
    rank = basis_ref.shape[0]
    sd = source_layers(sd_ref, k, width)
    first = lax.axis_index("depth") * nz
    above = sd < first
    for n in range(blocks):
        lanes = slice(n * width, (n + 1) * width)
        model = model_ref[:, lanes]
        coef = rate_ref[:, lanes] * (1.0 / depth_count) * jnp.exp(0.5 * model)
        decay = jnp.exp(-coef)
        w = w_ref[:, lanes]
        entering = got_ref[n, 0:k, :]
        f = jnp.where(above, entering, 0.0)
        products = []
        for z in range(nz):
            f = decay[z : z + 1] * f + jnp.where(sd == first + z, w, 0.0)
            products.append(f * (f - obs_ref[z, :, lanes]))
        deeper = jnp.where(above, 0.0, entering)
        below_sum = got_ref[n, k : k + 1, :]
        for z in reversed(range(nz)):
            deeper = deeper + products[z]
            data = jnp.sum(jnp.where(sd < first + z, deeper, 0.0), axis=0, keepdims=True) + below_sum
            gradient_ref[z : z + 1, lanes] = model[z : z + 1] - coef[z : z + 1] / k * data
    columns = model_ref.shape[1]
    grad = gradient_ref[...].astype(jnp.bfloat16).astype(f32)
    noise = noise_ref[...].astype(jnp.bfloat16).astype(f32)

    def fold(x):
        parts = [x[:, c : c + LANES] for c in range(0, columns, LANES)]
        while len(parts) > 1:
            parts = [a + b for a, b in zip(parts[::2], parts[1::2])] + parts[len(parts) & ~1 :]
        return parts[0]

    def project(step, _):
        for i in range(4):
            r = step * 4 + i
            line = basis_ref[r].astype(f32)
            sums_ref[0, r] = fold(line * grad)
            sums_ref[1, r] = fold(line * noise)
        return 0

    lax.fori_loop(0, rank // 4, project, 0)
    for which in range(2):
        lanesums = jnp.sum(sums_ref[which], axis=1)
        line = jnp.sum(lanesums.T, axis=0, keepdims=True)
        for n in range(blocks):
            out_ref[n, which : which + 1, :] = line


def proposal_kernel(
    depth_count, sd_ref, got_ref, curvature_ref, gradient_ref, model_ref, rate_ref, w_ref, obs_ref,
    noise_ref, basis_ref, proposal_ref, out_ref, energy_ref, mix_ref
):
    blocks, width = out_ref.shape[0], out_ref.shape[2]
    nz, columns = model_ref.shape
    k = w_ref.shape[0]
    rank = basis_ref.shape[0]
    projected = got_ref[0, 0:2, :]
    for n in range(1, blocks):
        projected = projected + got_ref[n, 0:2, :]
    curvature = curvature_ref[...]
    damping = curvature / (1.0 + curvature)
    shrink = 1.0 - 1.0 / jnp.sqrt(1.0 + curvature)
    mix = (damping * projected[0:1] - shrink * projected[1:2]).astype(jnp.bfloat16).astype(f32)
    mix_ref[...] = jnp.broadcast_to(mix, (LANES, rank)).T

    def correct(step, sums):
        for i in range(4):
            r = step * 4 + i
            weight = mix_ref[pl.ds(r, 1), :]
            weight = jnp.broadcast_to(weight, (nz, LANES))
            line = basis_ref[r].astype(f32)
            sums = tuple(
                s + line[:, c * LANES : (c + 1) * LANES] * weight for c, s in enumerate(sums)
            )
        return sums

    zero = jnp.zeros((nz, LANES), f32)
    sums = lax.fori_loop(0, rank // 4, correct, (zero,) * (columns // LANES))
    for c, s in enumerate(sums):
        at = slice(c * LANES, (c + 1) * LANES)
        proposal_ref[:, at] = model_ref[:, at] - gradient_ref[:, at] + noise_ref[:, at] + s

    sd = source_layers(sd_ref, k, width)
    first = lax.axis_index("depth") * nz
    energy = jnp.zeros((1, 1), f32)
    for n in range(blocks):
        lanes = slice(n * width, (n + 1) * width)
        model = proposal_ref[:, lanes]
        coef = rate_ref[:, lanes] * (1.0 / depth_count) * jnp.exp(0.5 * model)
        rows, through, squares, part = summarize(coef, w_ref[:, lanes], sd, first, obs_ref, lanes)
        write_summary(out_ref, n, rows, through, squares)
        energy = energy + total(part) / k + 0.5 * total(model * model)
    energy_ref[...] = jnp.broadcast_to(energy, energy_ref.shape)


def energy_kernel(nz, sd_ref, got_ref, first_ref, owner_ref, next_ref, out_ref):
    blocks, _, width = got_ref.shape
    k = sd_ref.shape[0]
    sd = source_layers(sd_ref, k, width)
    _, energy = scan_slabs(sd, nz, got_ref)
    drop = first_ref[...] + owner_ref[...] - next_ref[...] - total(energy) / k
    for n in range(blocks):
        out_ref[n] = drop


def final_kernel(cells, got_ref, out_ref):
    drop = got_ref[0]
    for n in range(1, got_ref.shape[0]):
        drop = drop + got_ref[n]
    out_ref[...] = drop[0:1, 0:1] / cells


def call(kernel, out_shape, in_smem, *args, scratch=(), flops=1000, out_specs=None):
    vmem = pl.BlockSpec(memory_space=pltpu.VMEM)
    smem = pl.BlockSpec(memory_space=pltpu.SMEM)
    many = isinstance(out_shape, (list, tuple))
    return pl.pallas_call(
        kernel,
        out_shape=out_shape,
        in_specs=[smem if i in in_smem else vmem for i in range(len(args))],
        out_specs=[vmem] * len(out_shape) if many else vmem,
        scratch_shapes=scratch,
        compiler_params=pltpu.CompilerParams(vmem_limit_bytes=24 * 2**20),
        cost_estimate=pl.CostEstimate(flops=flops, bytes_accessed=flops, transcendentals=0),
    )(*args)


def local(model_field, column_rate, wavelets, source_depth, observed, basis, curvature, noise_draw):
    slabs = lax.axis_size("depth")
    nz, columns = model_field.shape
    sources = wavelets.shape[0]
    rank = basis.shape[0]
    depth_count = nz * slabs
    width = columns // slabs
    rate = column_rate.reshape(1, columns)
    bends = curvature.reshape(1, rank)
    struct = jax.ShapeDtypeStruct
    summary = struct((slabs, pad_rows(sources + 2), width), f32)
    scalar = struct((8, LANES), f32)

    def exchange(x):
        return lax.all_to_all(x, "depth", 0, 0)

    sent, energy_first = call(
        functools.partial(first_kernel, depth_count), [summary, scalar], (0,),
        source_depth, model_field, rate, wavelets, observed,
    )
    got = exchange(sent)
    sent, energy_owner = call(
        functools.partial(owner_kernel, nz), [struct((slabs, pad_rows(sources + 1), width), f32), scalar], (0,),
        source_depth, got,
    )
    got = exchange(sent)
    gradient, sent = call(
        functools.partial(gradient_kernel, depth_count),
        [struct((nz, columns), f32), struct((slabs, 8, rank), f32)], (0,),
        source_depth, got, model_field, rate, wavelets, observed, noise_draw, basis,
        scratch=[pltpu.VMEM((2, rank, nz, LANES), f32)],
    )
    got = exchange(sent)
    proposal, sent, energy_next = call(
        functools.partial(proposal_kernel, depth_count),
        [struct((nz, columns), f32), summary, scalar], (0,),
        source_depth, got, bends, gradient, model_field, rate, wavelets, observed, noise_draw, basis,
        scratch=[pltpu.VMEM((rank, LANES), f32)],
    )
    got = exchange(sent)
    sent = call(
        functools.partial(energy_kernel, nz), struct((slabs, 8, LANES), f32), (0,),
        source_depth, got, energy_first, energy_owner, energy_next,
    )
    got = exchange(sent)
    gain = call(functools.partial(final_kernel, depth_count * columns), struct((1, 1), f32), (), got)
    return (proposal, gain.reshape(1))


def solution(mesh):
    in_specs = (
        P(("chain", "depth"), None),
        P("chain"),
        P("chain", None),
        P("chain"),
        P(("chain", "depth"), None, None),
        P("chain", "depth", None),
        P("chain"),
        P(("chain", "depth"), None),
    )
    out_specs = (P(("chain", "depth"), None), P("chain"))
    return jax.shard_map(local, mesh=mesh, in_specs=in_specs, out_specs=out_specs, check_vma=False)
```

```python
import functools

import jax
import jax.numpy as jnp
from jax import lax
from jax.experimental import pallas as pl
from jax.experimental.pallas import tpu as pltpu
from jax.sharding import PartitionSpec as P

LANES = 128
f32 = jnp.float32


def pad_rows(rows):
    return -(-rows // 8) * 8


def source_layers(sd_ref, count):
    row = lax.broadcasted_iota(jnp.int32, (count, LANES), 0)
    layers = jnp.zeros((count, LANES), jnp.int32)
    for k in range(count):
        layers = jnp.where(row == k, sd_ref[k], layers)
    return layers


def widen(layers_ref, width):
    layers = layers_ref[...]
    if width % LANES == 0:
        return jnp.concatenate([layers] * (width // LANES), axis=1)
    return layers[:, :width]


def split(width):
    return (width // LANES, LANES) if width % LANES == 0 else (1, width)


def wide(ref, n, start, count, parts):
    pieces = [ref[n, parts * start + p * count : parts * start + (p + 1) * count, :] for p in range(parts)]
    return pieces[0] if parts == 1 else jnp.concatenate(pieces, axis=1)


def put_wide(ref, n, start, value, parts):
    count, lanes = value.shape[0], value.shape[1] // parts
    for p in range(parts):
        ref[n, parts * start + p * count : parts * start + (p + 1) * count, :] = value[:, p * lanes : (p + 1) * lanes]


def summarize(coef, w, sd, first, obs_ref, lanes):
    nz = coef.shape[0]
    decay = jnp.exp(-coef)
    above = sd < first
    f = jnp.where(above, 1.0, 0.0)
    through = jnp.ones((1, coef.shape[1]), f32)
    squares = jnp.zeros_like(through)
    cross = jnp.zeros_like(w)
    own = jnp.zeros_like(w)
    for z in range(nz):
        step = decay[z : z + 1]
        f = step * f + jnp.where(sd == first + z, w, 0.0)
        through = through * step
        squares = squares + through * through
        cross = cross + f * obs_ref[z, :, lanes]
        own = own + f * f
    rows = jnp.where(above, cross, f)
    part = jnp.where(above, 0.0, own - 2.0 * cross)
    return rows, through, squares, part


def total(x):
    return jnp.sum(jnp.sum(x, axis=0, keepdims=True), axis=1, keepdims=True)


def write_summary(out_ref, n, rows, through, squares, parts):
    k = rows.shape[0]
    put_wide(out_ref, n, 0, rows, parts)
    put_wide(out_ref, n, k, through, parts)
    put_wide(out_ref, n, k + 1, squares, parts)


def first_kernel(
    depth_count, blocks, sd_hbm, model_hbm, rate_hbm, w_hbm, obs_hbm, noise_hbm, curvature_hbm,
    out_ref, energy_ref, layers_ref, model_ref, rate_ref, w_ref, obs_ref, noise_ref, curvature_ref,
    sd_ref, sems, obs_sems
):
    nz, columns = model_ref.shape
    k = w_ref.shape[0]
    width = columns // blocks
    parts = split(width)[0]
    copies = [
        pltpu.make_async_copy(src, dst, sems.at[i])
        for i, (src, dst) in enumerate([
            (sd_hbm, sd_ref), (model_hbm, model_ref), (rate_hbm, rate_ref), (w_hbm, w_ref),
            (noise_hbm, noise_ref), (curvature_hbm, curvature_ref),
        ])
    ]
    pieces = obs_sems.shape[0]
    piece = columns // pieces
    obs_copies = []
    for i in range(pieces):
        at = pl.ds(i * piece, piece)
        obs_copies.append(pltpu.make_async_copy(obs_hbm.at[:, :, at], obs_ref.at[:, :, at], obs_sems.at[i]))
    for copy in copies[:4]:
        copy.start()
    for copy in obs_copies:
        copy.start()
    for copy in copies[4:]:
        copy.start()
    for copy in copies[:4]:
        copy.wait()
    layers_ref[...] = source_layers(sd_ref, k)
    sd = widen(layers_ref, width)
    first = lax.axis_index("depth") * nz
    energy = jnp.zeros((1, 1), f32)
    arrived = 0
    for n in range(blocks):
        while arrived * piece < (n + 1) * width:
            obs_copies[arrived].wait()
            arrived += 1
        lanes = slice(n * width, (n + 1) * width)
        model = model_ref[:, lanes]
        coef = rate_ref[:, lanes] * (1.0 / depth_count) * jnp.exp(0.5 * model)
        rows, through, squares, part = summarize(coef, w_ref[:, lanes], sd, first, obs_ref, lanes)
        write_summary(out_ref, n, rows, through, squares, parts)
        energy = energy + total(part) / k + 0.5 * total(model * model)
    energy_ref[...] = jnp.broadcast_to(energy, energy_ref.shape)
    for copy in copies[4:]:
        copy.wait()


def project(vectors, basis_ref, rows, full_ref):
    full_ref[rows, :] = lax.dot_general(
        basis_ref[rows, :], vectors, (((1,), (1,)), ((), ())), preferred_element_type=f32
    )


def directions(full_ref, nz):
    rank = full_ref.shape[0] // nz
    lane = lax.broadcasted_iota(jnp.int32, (rank, nz), 1)
    picked = jnp.zeros((rank, nz), f32)
    for z in range(nz):
        picked = jnp.where(lane == z, full_ref[pl.ds(z, rank, stride=nz), :], picked)
    ones = jnp.ones((8, nz), f32)
    return lax.dot_general(
        ones, picked, (((1,), (1,)), ((), ())), precision=lax.Precision.HIGHEST, preferred_element_type=f32
    )[0:1]


def stream(basis_hbm, basis_ref, sems):
    pieces = sems.shape[0]
    piece = basis_ref.shape[0] // pieces
    started = []
    for i in range(pieces):
        rows = pl.ds(i * piece, piece)
        copy = pltpu.make_async_copy(basis_hbm.at[rows, :], basis_ref.at[rows, :], sems.at[i])
        copy.start()
        started.append((rows, copy))
    return started


def noise_kernel(nz, basis_hbm, noise_ref, q_ref, basis_ref, full_ref, sems):
    vectors = noise_ref[...].astype(jnp.bfloat16)
    for rows, copy in stream(basis_hbm, basis_ref, sems):
        copy.wait()
        project(vectors, basis_ref, rows, full_ref)
    q_ref[...] = directions(full_ref, nz)


def scan_slabs(sd, nz, got_ref, parts):
    blocks = got_ref.shape[0]
    k = sd.shape[0]
    carry = jnp.zeros(sd.shape, f32)
    energy = jnp.zeros(sd.shape, f32)
    carries = []
    for n in range(blocks):
        rows = wide(got_ref, n, 0, k, parts)
        through = wide(got_ref, n, k, 1, parts)
        squares = wide(got_ref, n, k + 1, 1, parts)
        carries.append(carry)
        energy = energy + carry * (carry * squares - 2.0 * rows)
        carry = through * carry + jnp.where(sd >= n * nz, rows, 0.0)
    return carries, energy


def owner_kernel(nz, width, layers_ref, got_ref, out_ref, energy_ref):
    blocks = got_ref.shape[0]
    parts = split(width)[0]
    k = layers_ref.shape[0]
    sd = widen(layers_ref, width)
    carries, energy = scan_slabs(sd, nz, got_ref, parts)
    deeper = jnp.zeros(sd.shape, f32)
    for n in reversed(range(blocks)):
        above = sd < n * nz
        put_wide(out_ref, n, 0, jnp.where(above, carries[n], deeper), parts)
        put_wide(out_ref, n, k, jnp.sum(jnp.where(above, deeper, 0.0), axis=0, keepdims=True), parts)
        rows = wide(got_ref, n, 0, k, parts)
        squares = wide(got_ref, n, k + 1, 1, parts)
        deeper = deeper + carries[n] * (carries[n] * squares - rows)
    energy_ref[...] = jnp.broadcast_to(total(energy) / k, energy_ref.shape)


def gradient_kernel(
    depth_count, layers_ref, got_ref, model_ref, rate_ref, w_ref, obs_ref, q_ref, basis_hbm,
    gradient_ref, out_ref, basis_ref, spread_ref, full_ref, sems
):
    started = stream(basis_hbm, basis_ref, sems)
    blocks = got_ref.shape[0]
    nz, columns = model_ref.shape
    width = columns // blocks
    parts = split(width)[0]
    k = w_ref.shape[0]
    sd = widen(layers_ref, width)
    first = lax.axis_index("depth") * nz
    above = sd < first
    for n in range(blocks):
        lanes = slice(n * width, (n + 1) * width)
        model = model_ref[:, lanes]
        coef = rate_ref[:, lanes] * (1.0 / depth_count) * jnp.exp(0.5 * model)
        decay = jnp.exp(-coef)
        w = w_ref[:, lanes]
        entering = wide(got_ref, n, 0, k, parts)
        f = jnp.where(above, entering, 0.0)
        products = []
        for z in range(nz):
            f = decay[z : z + 1] * f + jnp.where(sd == first + z, w, 0.0)
            products.append(f * (f - obs_ref[z, :, lanes]))
        deeper = jnp.where(above, 0.0, entering)
        below_sum = wide(got_ref, n, k, 1, parts)
        for z in reversed(range(nz)):
            deeper = deeper + products[z]
            data = jnp.sum(jnp.where(sd < first + z, deeper, 0.0), axis=0, keepdims=True) + below_sum
            gradient_ref[z : z + 1, lanes] = model[z : z + 1] - coef[z : z + 1] / k * data
    row = lax.broadcasted_iota(jnp.int32, spread_ref.shape, 0)
    column = lax.broadcasted_iota(jnp.int32, spread_ref.shape, 1)
    spread_ref[...] = jnp.where(row == column // nz, 1.0, 0.0).astype(jnp.bfloat16)
    vectors = gradient_ref[...].astype(jnp.bfloat16)
    for rows, copy in started:
        copy.wait()
        project(vectors, basis_ref, rows, full_ref)
    line = directions(full_ref, nz)
    for n in range(blocks):
        out_ref[n, 0:1, :] = line
        out_ref[n, 1:2, :] = q_ref[...]


def proposal_kernel(
    depth_count, width, layers_ref, got_ref, curvature_ref, gradient_ref, model_ref, rate_ref, w_ref,
    obs_ref, noise_ref, basis_ref, spread_ref, proposal_ref, out_ref, energy_ref
):
    blocks = out_ref.shape[0]
    parts = split(width)[0]
    nz, columns = model_ref.shape
    k = w_ref.shape[0]
    rank, total_rows = spread_ref.shape
    projected = got_ref[0, 0:2, :]
    for n in range(1, blocks):
        projected = projected + got_ref[n, 0:2, :]
    curvature = curvature_ref[...]
    damping = curvature / (1.0 + curvature)
    shrink = 1.0 - 1.0 / jnp.sqrt(1.0 + curvature)
    mix = (damping * projected[0:1] - shrink * projected[1:2]).astype(jnp.bfloat16)
    spread = jnp.dot(jnp.broadcast_to(mix, (nz, rank)), spread_ref[...], preferred_element_type=f32)
    row = lax.broadcasted_iota(jnp.int32, (nz, total_rows), 0)
    column = lax.broadcasted_iota(jnp.int32, (nz, total_rows), 1)
    weights = jnp.where(row == column % nz, spread, 0.0).astype(jnp.bfloat16)
    correction = jnp.dot(weights, basis_ref[...], preferred_element_type=f32)
    proposal_ref[...] = model_ref[...] - gradient_ref[...] + noise_ref[...] + correction

    sd = widen(layers_ref, width)
    first = lax.axis_index("depth") * nz
    energy = jnp.zeros((1, 1), f32)
    for n in range(blocks):
        lanes = slice(n * width, (n + 1) * width)
        model = proposal_ref[:, lanes]
        coef = rate_ref[:, lanes] * (1.0 / depth_count) * jnp.exp(0.5 * model)
        rows, through, squares, part = summarize(coef, w_ref[:, lanes], sd, first, obs_ref, lanes)
        write_summary(out_ref, n, rows, through, squares, parts)
        energy = energy + total(part) / k + 0.5 * total(model * model)
    energy_ref[...] = jnp.broadcast_to(energy, energy_ref.shape)


def energy_kernel(nz, width, layers_ref, got_ref, first_ref, owner_ref, next_ref, out_ref):
    blocks = got_ref.shape[0]
    k = layers_ref.shape[0]
    sd = widen(layers_ref, width)
    _, energy = scan_slabs(sd, nz, got_ref, split(width)[0])
    drop = first_ref[...] + owner_ref[...] - next_ref[...] - total(energy) / k
    for n in range(blocks):
        out_ref[n] = drop


def final_kernel(cells, got_ref, out_ref):
    drop = got_ref[0]
    for n in range(1, got_ref.shape[0]):
        drop = drop + got_ref[n]
    out_ref[...] = drop[0:1, 0:1] / cells


def call(kernel, outs, args, hbm=(), scratch=(), flops=10**6, limit=16):
    vmem = pl.BlockSpec(memory_space=pltpu.VMEM)
    far = pl.BlockSpec(memory_space=pltpu.HBM)
    args = [pltpu.with_memory_space_constraint(x, pltpu.HBM) if i in hbm else x for i, x in enumerate(args)]
    return pl.pallas_call(
        kernel,
        out_shape=outs,
        in_specs=[far if i in hbm else vmem for i in range(len(args))],
        out_specs=[vmem] * len(outs),
        scratch_shapes=scratch,
        compiler_params=pltpu.CompilerParams(vmem_limit_bytes=limit * 2**20),
        cost_estimate=pl.CostEstimate(flops=flops, bytes_accessed=flops, transcendentals=0),
    )(*args)


def local(model_field, column_rate, wavelets, source_depth, observed, basis, curvature, noise_draw):
    slabs = lax.axis_size("depth")
    nz, columns = model_field.shape
    sources = wavelets.shape[0]
    rank = basis.shape[0]
    depth_count = nz * slabs
    width = columns // slabs
    parts, lanes = split(width)
    struct = jax.ShapeDtypeStruct
    summary = struct((slabs, pad_rows(parts * (sources + 2)), lanes), f32)
    answer = struct((slabs, pad_rows(parts * (sources + 1)), lanes), f32)
    scalar = struct((8, LANES), f32)
    field = struct((nz, columns), f32)
    dma = pltpu.SemaphoreType.DMA

    def exchange(x):
        return lax.all_to_all(x, "depth", 0, 0)

    sent, energy_first, layers, model, rate, w, obs, noise, bends = call(
        functools.partial(first_kernel, depth_count, slabs),
        [summary, scalar, struct((sources, LANES), jnp.int32), field, struct((1, columns), f32),
         struct(wavelets.shape, f32), struct(observed.shape, f32), field, struct((1, rank), f32)],
        [source_depth, model_field, column_rate.reshape(1, columns), wavelets, observed, noise_draw,
         curvature.reshape(1, rank)],
        hbm=range(7),
        scratch=[pltpu.SMEM((sources,), jnp.int32), dma((6,)), dma((8,))],
    )
    got = exchange(sent)
    flat = basis.reshape(rank * nz, columns)
    buffers = [pltpu.VMEM((rank * nz, nz), f32), dma((8,))]
    (q,) = call(
        functools.partial(noise_kernel, nz), [struct((1, rank), f32)], [flat, noise], hbm=(0,),
        scratch=[pltpu.VMEM(flat.shape, flat.dtype)] + buffers, flops=10**8, limit=24,
    )
    sent, energy_owner = call(
        functools.partial(owner_kernel, nz, width), [answer, scalar], [layers, got],
    )
    got = exchange(sent)
    gradient, sent, near, spread = call(
        functools.partial(gradient_kernel, depth_count),
        [field, struct((slabs, 8, rank), f32), struct(flat.shape, flat.dtype),
         struct((rank, rank * nz), jnp.bfloat16)],
        [layers, got, model, rate, w, obs, q, flat], hbm=(7,), scratch=buffers, limit=24,
    )
    got = exchange(sent)
    proposal, sent, energy_next = call(
        functools.partial(proposal_kernel, depth_count, width),
        [field, summary, scalar],
        [layers, got, bends, gradient, model, rate, w, obs, noise, near, spread], limit=24,
    )
    got = exchange(sent)
    (sent,) = call(
        functools.partial(energy_kernel, nz, width), [struct((slabs, 8, LANES), f32)],
        [layers, got, energy_first, energy_owner, energy_next],
    )
    got = exchange(sent)
    (gain,) = call(functools.partial(final_kernel, depth_count * columns), [struct((1, 1), f32)], [got])
    return (proposal, gain.reshape(1))


def solution(mesh):
    in_specs = (
        P(("chain", "depth"), None),
        P("chain"),
        P("chain", None),
        P("chain"),
        P(("chain", "depth"), None, None),
        P("chain", "depth", None),
        P("chain"),
        P(("chain", "depth"), None),
    )
    out_specs = (P(("chain", "depth"), None), P("chain"))
    return jax.shard_map(local, mesh=mesh, in_specs=in_specs, out_specs=out_specs, check_vma=False)
```

```python
import functools

import jax
import jax.numpy as jnp
from jax import lax
from jax.experimental import pallas as pl
from jax.experimental.pallas import tpu as pltpu
from jax.sharding import PartitionSpec as P

LANES = 128
f32 = jnp.float32


def pad_rows(rows):
    return -(-rows // 8) * 8


def source_layers(sd_ref, count):
    row = lax.broadcasted_iota(jnp.int32, (count, LANES), 0)
    layers = jnp.zeros((count, LANES), jnp.int32)
    for k in range(count):
        layers = jnp.where(row == k, sd_ref[k], layers)
    return layers


def widen(layers_ref, width):
    layers = layers_ref[...]
    if width % LANES == 0:
        return jnp.concatenate([layers] * (width // LANES), axis=1)
    return layers[:, :width]


def split(width):
    return (width // LANES, LANES) if width % LANES == 0 else (1, width)


def wide(ref, n, start, count, parts):
    pieces = [ref[n, parts * start + p * count : parts * start + (p + 1) * count, :] for p in range(parts)]
    return pieces[0] if parts == 1 else jnp.concatenate(pieces, axis=1)


def put_wide(ref, n, start, value, parts):
    count, lanes = value.shape[0], value.shape[1] // parts
    for p in range(parts):
        ref[n, parts * start + p * count : parts * start + (p + 1) * count, :] = value[:, p * lanes : (p + 1) * lanes]


def summarize(coef, w, sd, first, obs_ref, lanes):
    nz = coef.shape[0]
    decay = jnp.exp(-coef)
    above = sd < first
    f = jnp.where(above, 1.0, 0.0)
    through = jnp.ones((1, coef.shape[1]), f32)
    squares = jnp.zeros_like(through)
    cross = jnp.zeros_like(w)
    own = jnp.zeros_like(w)
    for z in range(nz):
        step = decay[z : z + 1]
        f = step * f + jnp.where(sd == first + z, w, 0.0)
        through = through * step
        squares = squares + through * through
        cross = cross + f * obs_ref[z, :, lanes]
        own = own + f * f
    rows = jnp.where(above, cross, f)
    part = jnp.where(above, 0.0, own - 2.0 * cross)
    return rows, through, squares, part


def total(x):
    return jnp.sum(jnp.sum(x, axis=0, keepdims=True), axis=1, keepdims=True)


def write_summary(out_ref, n, rows, through, squares, parts):
    k = rows.shape[0]
    put_wide(out_ref, n, 0, rows, parts)
    put_wide(out_ref, n, k, through, parts)
    put_wide(out_ref, n, k + 1, squares, parts)


def first_kernel(
    depth_count, blocks, sd_hbm, model_hbm, rate_hbm, w_hbm, obs_hbm, noise_hbm, curvature_hbm,
    out_ref, energy_ref, layers_ref, model_ref, rate_ref, w_ref, obs_ref, noise_ref, curvature_ref,
    sd_ref, sems, obs_sems
):
    nz, columns = model_ref.shape
    k = w_ref.shape[0]
    width = columns // blocks
    parts = split(width)[0]
    copies = [
        pltpu.make_async_copy(src, dst, sems.at[i])
        for i, (src, dst) in enumerate([
            (sd_hbm, sd_ref), (model_hbm, model_ref), (rate_hbm, rate_ref), (w_hbm, w_ref),
            (noise_hbm, noise_ref), (curvature_hbm, curvature_ref),
        ])
    ]
    pieces = obs_sems.shape[0]
    piece = columns // pieces
    obs_copies = []
    for i in range(pieces):
        at = pl.ds(i * piece, piece)
        obs_copies.append(pltpu.make_async_copy(obs_hbm.at[:, :, at], obs_ref.at[:, :, at], obs_sems.at[i]))
    for copy in copies[:4]:
        copy.start()
    for copy in obs_copies:
        copy.start()
    for copy in copies[4:]:
        copy.start()
    for copy in copies[:4]:
        copy.wait()
    layers_ref[...] = source_layers(sd_ref, k)
    sd = widen(layers_ref, width)
    first = lax.axis_index("depth") * nz
    for copy in obs_copies:
        copy.wait()
    misfit = jnp.zeros(sd.shape, f32)
    square = jnp.zeros((nz, width), f32)
    for n in range(blocks):
        lanes = slice(n * width, (n + 1) * width)
        model = model_ref[:, lanes]
        coef = rate_ref[:, lanes] * (1.0 / depth_count) * jnp.exp(0.5 * model)
        rows, through, squares, part = summarize(coef, w_ref[:, lanes], sd, first, obs_ref, lanes)
        write_summary(out_ref, n, rows, through, squares, parts)
        misfit = misfit + part
        square = square + model * model
    energy_ref[...] = jnp.broadcast_to(total(misfit) / k + 0.5 * total(square), energy_ref.shape)
    for copy in copies[4:]:
        copy.wait()


def group(nz, offset, expand):
    one = lax.broadcasted_iota(jnp.int32, (LANES, LANES), 1 - expand)
    each = lax.broadcasted_iota(jnp.int32, (LANES, LANES), expand)
    return jnp.where(one == each // nz + offset, 1.0, 0.0)


def exact_dot(a, b):
    return jnp.dot(a, b, precision=lax.Precision.HIGHEST, preferred_element_type=f32)


def project(vectors, basis_ref):
    return lax.dot_general(vectors, basis_ref, (((1,), (1,)), ((), ())), preferred_element_type=f32)


def own_layer(every, sums_ref):
    nz = every.shape[0]
    layer = lax.broadcasted_iota(jnp.int32, (nz, LANES), 0)
    lane = lax.broadcasted_iota(jnp.int32, (nz, LANES), 1)
    for t in range(every.shape[1] // LANES):
        mine = jnp.where(layer == lane % nz, every[:, t * LANES : (t + 1) * LANES], 0.0)
        sums_ref[t : t + 1, :] = jnp.sum(mine, axis=0, keepdims=True)


def stream(basis_hbm, basis_ref, sems):
    pieces = sems.shape[0]
    piece = basis_ref.shape[1] // pieces
    started = []
    for i in range(pieces):
        at = pl.ds(i * piece, piece)
        copy = pltpu.make_async_copy(basis_hbm.at[:, at], basis_ref.at[:, at], sems.at[i])
        copy.start()
        started.append((slice(i * piece, (i + 1) * piece), copy))
    return started


def noise_kernel(nz, basis_hbm, noise_ref, curvature_ref, q_ref, bends_ref, basis_ref, sums_ref, sems):
    started = stream(basis_hbm, basis_ref, sems)
    share = LANES // nz
    sums_ref[...] = jnp.zeros_like(sums_ref)
    for i in range(sums_ref.shape[0]):
        sums_ref[i : i + 1, 0:share] = curvature_ref[:, i * share : (i + 1) * share]
    bends_ref[...] = exact_dot(sums_ref[...], group(nz, 0, 1))
    vectors = noise_ref[...].astype(jnp.bfloat16)
    every = jnp.zeros((nz, basis_ref.shape[0]), f32)
    for at, copy in started:
        copy.wait()
        every = every + project(vectors[:, at], basis_ref[:, at])
    own_layer(every, sums_ref)
    q_ref[...] = exact_dot(sums_ref[...], group(nz, share, 0))


def scan_slabs(sd, nz, got_ref, parts):
    blocks = got_ref.shape[0]
    k = sd.shape[0]
    carry = jnp.zeros(sd.shape, f32)
    energy = jnp.zeros(sd.shape, f32)
    carries = []
    for n in range(blocks):
        rows = wide(got_ref, n, 0, k, parts)
        through = wide(got_ref, n, k, 1, parts)
        squares = wide(got_ref, n, k + 1, 1, parts)
        carries.append(carry)
        energy = energy + carry * (carry * squares - 2.0 * rows)
        carry = through * carry + jnp.where(sd >= n * nz, rows, 0.0)
    return carries, energy


def owner_kernel(nz, width, layers_ref, got_ref, q_in, bends_in, out_ref, energy_ref, q_ref, bends_ref):
    blocks = got_ref.shape[0]
    parts = split(width)[0]
    k = layers_ref.shape[0]
    sd = widen(layers_ref, width)
    carries, energy = scan_slabs(sd, nz, got_ref, parts)
    deeper = jnp.zeros(sd.shape, f32)
    for n in reversed(range(blocks)):
        above = sd < n * nz
        put_wide(out_ref, n, 0, jnp.where(above, carries[n], deeper), parts)
        put_wide(out_ref, n, k, jnp.sum(jnp.where(above, deeper, 0.0), axis=0, keepdims=True), parts)
        rows = wide(got_ref, n, 0, k, parts)
        squares = wide(got_ref, n, k + 1, 1, parts)
        deeper = deeper + carries[n] * (carries[n] * squares - rows)
    energy_ref[...] = jnp.broadcast_to(total(energy) / k, energy_ref.shape)
    q_ref[...] = q_in[...]
    bends_ref[...] = bends_in[...]


def gradient_kernel(
    depth_count, layers_ref, got_ref, model_ref, rate_ref, w_ref, obs_ref, q_ref, basis_hbm,
    gradient_ref, out_ref, basis_ref, sums_ref, sems
):
    started = stream(basis_hbm, basis_ref, sems)
    blocks = got_ref.shape[0]
    nz, columns = model_ref.shape
    width = columns // blocks
    parts = split(width)[0]
    k = w_ref.shape[0]
    sd = widen(layers_ref, width)
    first = lax.axis_index("depth") * nz
    above = sd < first
    for n in range(blocks):
        lanes = slice(n * width, (n + 1) * width)
        model = model_ref[:, lanes]
        coef = rate_ref[:, lanes] * (1.0 / depth_count) * jnp.exp(0.5 * model)
        decay = jnp.exp(-coef)
        w = w_ref[:, lanes]
        entering = wide(got_ref, n, 0, k, parts)
        f = jnp.where(above, entering, 0.0)
        products = []
        for z in range(nz):
            f = decay[z : z + 1] * f + jnp.where(sd == first + z, w, 0.0)
            products.append(f * (f - obs_ref[z, :, lanes]))
        deeper = jnp.where(above, 0.0, entering)
        below_sum = wide(got_ref, n, k, 1, parts)
        for z in reversed(range(nz)):
            deeper = deeper + products[z]
            data = jnp.sum(jnp.where(sd < first + z, deeper, 0.0), axis=0, keepdims=True) + below_sum
            gradient_ref[z : z + 1, lanes] = model[z : z + 1] - coef[z : z + 1] / k * data
    vectors = gradient_ref[...].astype(jnp.bfloat16)
    every = jnp.zeros((nz, basis_ref.shape[0]), f32)
    for at, copy in started:
        copy.wait()
        every = every + project(vectors[:, at], basis_ref[:, at])
    own_layer(every, sums_ref)
    both = exact_dot(sums_ref[...], group(nz, 0, 0)) + q_ref[...]
    for n in range(blocks):
        out_ref[n] = both


def proposal_kernel(
    depth_count, width, layers_ref, got_ref, bends_ref, gradient_ref, model_ref, rate_ref, w_ref,
    obs_ref, noise_ref, basis_ref, proposal_ref, out_ref, energy_ref
):
    blocks = out_ref.shape[0]
    parts = split(width)[0]
    nz, columns = model_ref.shape
    k = w_ref.shape[0]
    projected = got_ref[0]
    for n in range(1, blocks):
        projected = projected + got_ref[n]
    p = exact_dot(projected, group(nz, 0, 1))
    q = exact_dot(projected, group(nz, LANES // nz, 1))
    curvature = bends_ref[...]
    damping = curvature / (1.0 + curvature)
    shrink = 1.0 - 1.0 / jnp.sqrt(1.0 + curvature)
    mix = (damping * p - shrink * q).astype(jnp.bfloat16).astype(f32)
    layer = lax.broadcasted_iota(jnp.int32, (nz, LANES), 0)
    lane = lax.broadcasted_iota(jnp.int32, (nz, LANES), 1)
    weights = jnp.concatenate(
        [jnp.where(layer == lane % nz, mix[i : i + 1, :], 0.0) for i in range(mix.shape[0])], axis=1
    ).astype(jnp.bfloat16)
    sd = widen(layers_ref, width)
    first = lax.axis_index("depth") * nz
    misfit = jnp.zeros(sd.shape, f32)
    square = jnp.zeros((nz, width), f32)
    for n in range(blocks):
        lanes = slice(n * width, (n + 1) * width)
        correction = jnp.dot(weights, basis_ref[:, lanes], preferred_element_type=f32)
        model = model_ref[:, lanes] - gradient_ref[:, lanes] + noise_ref[:, lanes] + correction
        proposal_ref[:, lanes] = model
        coef = rate_ref[:, lanes] * (1.0 / depth_count) * jnp.exp(0.5 * model)
        rows, through, squares, part = summarize(coef, w_ref[:, lanes], sd, first, obs_ref, lanes)
        write_summary(out_ref, n, rows, through, squares, parts)
        misfit = misfit + part
        square = square + model * model
    energy_ref[...] = jnp.broadcast_to(total(misfit) / k + 0.5 * total(square), energy_ref.shape)


def energy_kernel(nz, width, layers_ref, got_ref, first_ref, owner_ref, next_ref, out_ref):
    blocks = got_ref.shape[0]
    k = layers_ref.shape[0]
    sd = widen(layers_ref, width)
    _, energy = scan_slabs(sd, nz, got_ref, split(width)[0])
    drop = first_ref[...] + owner_ref[...] - next_ref[...] - total(energy) / k
    for n in range(blocks):
        out_ref[n] = drop


def final_kernel(cells, got_ref, out_ref):
    drop = got_ref[0]
    for n in range(1, got_ref.shape[0]):
        drop = drop + got_ref[n]
    out_ref[...] = drop[0:1, 0:1] / cells


def call(kernel, outs, args, hbm=(), scratch=(), flops=10**6, limit=16):
    vmem = pl.BlockSpec(memory_space=pltpu.VMEM)
    far = pl.BlockSpec(memory_space=pltpu.HBM)
    args = [pltpu.with_memory_space_constraint(x, pltpu.HBM) if i in hbm else x for i, x in enumerate(args)]
    return pl.pallas_call(
        kernel,
        out_shape=outs,
        in_specs=[far if i in hbm else vmem for i in range(len(args))],
        out_specs=[vmem] * len(outs),
        scratch_shapes=scratch,
        compiler_params=pltpu.CompilerParams(vmem_limit_bytes=limit * 2**20),
        cost_estimate=pl.CostEstimate(flops=flops, bytes_accessed=flops, transcendentals=0),
    )(*args)


def local(model_field, column_rate, wavelets, source_depth, observed, basis, curvature, noise_draw):
    slabs = lax.axis_size("depth")
    nz, columns = model_field.shape
    sources = wavelets.shape[0]
    rank = basis.shape[0]
    depth_count = nz * slabs
    width = columns // slabs
    parts, lanes = split(width)
    struct = jax.ShapeDtypeStruct
    summary = struct((slabs, pad_rows(parts * (sources + 2)), lanes), f32)
    answer = struct((slabs, pad_rows(parts * (sources + 1)), lanes), f32)
    scalar = struct((8, LANES), f32)
    field = struct((nz, columns), f32)
    dma = pltpu.SemaphoreType.DMA

    def exchange(x):
        return lax.all_to_all(x, "depth", 0, 0)

    sent, energy_first, layers, model, rate, w, obs, noise, curved = call(
        functools.partial(first_kernel, depth_count, slabs),
        [summary, scalar, struct((sources, LANES), jnp.int32), field, struct((1, columns), f32),
         struct(wavelets.shape, f32), struct(observed.shape, f32), field, struct((1, rank), f32)],
        [source_depth, model_field, column_rate.reshape(1, columns), wavelets, observed, noise_draw,
         curvature.reshape(1, rank)],
        hbm=range(7),
        scratch=[pltpu.SMEM((sources,), jnp.int32), dma((6,)), dma((8,))],
    )
    got = exchange(sent)
    flat = basis.reshape(rank * nz, columns)
    sums = (rank * nz // LANES, LANES)
    buffers = [pltpu.VMEM(sums, f32), dma((8,))]
    q, bends = call(
        functools.partial(noise_kernel, nz), [struct(sums, f32)] * 2, [flat, noise, curved], hbm=(0,),
        scratch=[pltpu.VMEM(flat.shape, flat.dtype)] + buffers, flops=10**8, limit=24,
    )
    sent, energy_owner, q, bends = call(
        functools.partial(owner_kernel, nz, width), [answer, scalar] + [struct(sums, f32)] * 2,
        [layers, got, q, bends],
    )
    got = exchange(sent)
    gradient, sent, near = call(
        functools.partial(gradient_kernel, depth_count),
        [field, struct((slabs,) + sums, f32), struct(flat.shape, flat.dtype)],
        [layers, got, model, rate, w, obs, q, flat], hbm=(7,), scratch=buffers,
    )
    got = exchange(sent)
    proposal, sent, energy_next = call(
        functools.partial(proposal_kernel, depth_count, width),
        [field, summary, scalar],
        [layers, got, bends, gradient, model, rate, w, obs, noise, near],
    )
    got = exchange(sent)
    (sent,) = call(
        functools.partial(energy_kernel, nz, width), [struct((slabs, 8, LANES), f32)],
        [layers, got, energy_first, energy_owner, energy_next],
    )
    got = exchange(sent)
    (gain,) = call(functools.partial(final_kernel, depth_count * columns), [struct((1, 1), f32)], [got])
    return (proposal, gain.reshape(1))


def solution(mesh):
    in_specs = (
        P(("chain", "depth"), None),
        P("chain"),
        P("chain", None),
        P("chain"),
        P(("chain", "depth"), None, None),
        P("chain", "depth", None),
        P("chain"),
        P(("chain", "depth"), None),
    )
    out_specs = (P(("chain", "depth"), None), P("chain"))
    return jax.shard_map(local, mesh=mesh, in_specs=in_specs, out_specs=out_specs, check_vma=False)
```

```python
import functools

import jax
import jax.numpy as jnp
from jax import lax
from jax.experimental import pallas as pl
from jax.experimental.pallas import tpu as pltpu
from jax.sharding import PartitionSpec as P

LANES = 128
f32 = jnp.float32


def pad_rows(rows):
    return -(-rows // 8) * 8


def source_layers(sd_ref, count):
    row = lax.broadcasted_iota(jnp.int32, (count, LANES), 0)
    layers = jnp.zeros((count, LANES), jnp.int32)
    for k in range(count):
        layers = jnp.where(row == k, sd_ref[k], layers)
    return layers


def widen(layers_ref, width):
    layers = layers_ref[...]
    if width % LANES == 0:
        return jnp.concatenate([layers] * (width // LANES), axis=1)
    return layers[:, :width]


def split(width):
    return (width // LANES, LANES) if width % LANES == 0 else (1, width)


def wide(ref, n, start, count, parts):
    pieces = [ref[n, parts * start + p * count : parts * start + (p + 1) * count, :] for p in range(parts)]
    return pieces[0] if parts == 1 else jnp.concatenate(pieces, axis=1)


def put_wide(ref, n, start, value, parts):
    count, lanes = value.shape[0], value.shape[1] // parts
    for p in range(parts):
        ref[n, parts * start + p * count : parts * start + (p + 1) * count, :] = value[:, p * lanes : (p + 1) * lanes]


def summarize(coef, w, sd, first, obs_ref, lanes):
    nz = coef.shape[0]
    decay = jnp.exp(-coef)
    above = sd < first
    f = jnp.where(above, 1.0, 0.0)
    through = jnp.ones((1, coef.shape[1]), f32)
    squares = jnp.zeros_like(through)
    cross = jnp.zeros_like(w)
    own = jnp.zeros_like(w)
    for z in range(nz):
        step = decay[z : z + 1]
        f = step * f + jnp.where(sd == first + z, w, 0.0)
        through = through * step
        squares = squares + through * through
        cross = cross + f * obs_ref[z, :, lanes]
        own = own + f * f
    rows = jnp.where(above, cross, f)
    part = jnp.where(above, 0.0, own - 2.0 * cross)
    return rows, through, squares, part


def total(x):
    return jnp.sum(jnp.sum(x, axis=0, keepdims=True), axis=1, keepdims=True)


def write_summary(out_ref, n, rows, through, squares, parts):
    k = rows.shape[0]
    put_wide(out_ref, n, 0, rows, parts)
    put_wide(out_ref, n, k, through, parts)
    put_wide(out_ref, n, k + 1, squares, parts)


def expand(row, nz):
    rank, share = row.shape[1], LANES // nz
    line = lax.broadcasted_iota(jnp.int32, (rank // share, rank), 0)
    entry = lax.broadcasted_iota(jnp.int32, (rank // share, rank), 1)
    mine = jnp.where(entry // share == line, jnp.broadcast_to(row, line.shape), 0.0)
    entry = lax.broadcasted_iota(jnp.int32, (rank, LANES), 0)
    lane = lax.broadcasted_iota(jnp.int32, (rank, LANES), 1)
    pick = jnp.where(entry % share == lane // nz, 1.0, 0.0)
    return jnp.dot(mine, pick, precision=lax.Precision.HIGHEST, preferred_element_type=f32)


def first_kernel(
    depth_count, blocks, sd_hbm, model_hbm, rate_hbm, w_hbm, obs_hbm, noise_hbm, curvature_hbm,
    out_ref, energy_ref, layers_ref, model_ref, rate_ref, w_ref, obs_ref, noise_ref, bends_ref,
    curvature_ref, sd_ref, sems, obs_sems
):
    nz, columns = model_ref.shape
    k = w_ref.shape[0]
    width = columns // blocks
    parts = split(width)[0]
    copies = [
        pltpu.make_async_copy(src, dst, sems.at[i])
        for i, (src, dst) in enumerate([
            (curvature_hbm, curvature_ref), (sd_hbm, sd_ref), (model_hbm, model_ref), (rate_hbm, rate_ref),
            (w_hbm, w_ref), (noise_hbm, noise_ref),
        ])
    ]
    pieces = obs_sems.shape[0]
    piece = columns // pieces
    obs_copies = []
    for i in range(pieces):
        at = pl.ds(i * piece, piece)
        obs_copies.append(pltpu.make_async_copy(obs_hbm.at[:, :, at], obs_ref.at[:, :, at], obs_sems.at[i]))
    for copy in copies[:5]:
        copy.start()
    for copy in obs_copies:
        copy.start()
    copies[5].start()
    copies[0].wait()
    bends_ref[...] = expand(curvature_ref[...], nz)
    for copy in copies[1:5]:
        copy.wait()
    layers_ref[...] = source_layers(sd_ref, k)
    sd = widen(layers_ref, width)
    first = lax.axis_index("depth") * nz
    for copy in obs_copies:
        copy.wait()
    misfit = jnp.zeros(sd.shape, f32)
    square = jnp.zeros((nz, width), f32)
    for n in range(blocks):
        lanes = slice(n * width, (n + 1) * width)
        model = model_ref[:, lanes]
        coef = rate_ref[:, lanes] * (1.0 / depth_count) * jnp.exp(0.5 * model)
        rows, through, squares, part = summarize(coef, w_ref[:, lanes], sd, first, obs_ref, lanes)
        write_summary(out_ref, n, rows, through, squares, parts)
        misfit = misfit + part
        square = square + model * model
    energy_ref[...] = jnp.broadcast_to(total(misfit) / k + 0.5 * total(square), energy_ref.shape)
    copies[5].wait()


def group_sums(x, nz):
    step = 1
    while step < nz:
        x = x + pltpu.roll(x, step, 1)
        step *= 2
    return x


def spread(x, nz):
    lane = lax.broadcasted_iota(jnp.int32, x.shape, 1)
    x = jnp.where(lane % nz == nz - 1, x, 0.0)
    step = 1
    while step < nz:
        x = x + pltpu.roll(x, LANES - step, 1)
        step *= 2
    return x


def project(vectors, basis_ref):
    return lax.dot_general(vectors, basis_ref, (((1,), (1,)), ((), ())), preferred_element_type=f32)


def own_layer(every, sums_ref):
    nz = every.shape[0] // 2
    tiles = every.shape[1] // LANES
    layer = lax.broadcasted_iota(jnp.int32, (nz, LANES), 0)
    lane = lax.broadcasted_iota(jnp.int32, (nz, LANES), 1)
    own = layer == lane % nz
    for which in range(2):
        for t in range(tiles):
            mine = jnp.where(own, every[which * nz : (which + 1) * nz, t * LANES : (t + 1) * LANES], 0.0)
            at = which * tiles + t
            sums_ref[at : at + 1, :] = jnp.sum(mine, axis=0, keepdims=True)


def stream(basis_hbm, basis_ref, sems):
    pieces = sems.shape[0]
    piece = basis_ref.shape[1] // pieces
    started = []
    for i in range(pieces):
        at = pl.ds(i * piece, piece)
        copy = pltpu.make_async_copy(basis_hbm.at[:, at], basis_ref.at[:, at], sems.at[i])
        copy.start()
        started.append((slice(i * piece, (i + 1) * piece), copy))
    return started


def scan_slabs(sd, nz, got_ref, parts):
    blocks = got_ref.shape[0]
    k = sd.shape[0]
    carry = jnp.zeros(sd.shape, f32)
    energy = jnp.zeros(sd.shape, f32)
    carries = []
    for n in range(blocks):
        rows = wide(got_ref, n, 0, k, parts)
        through = wide(got_ref, n, k, 1, parts)
        squares = wide(got_ref, n, k + 1, 1, parts)
        carries.append(carry)
        energy = energy + carry * (carry * squares - 2.0 * rows)
        carry = through * carry + jnp.where(sd >= n * nz, rows, 0.0)
    return carries, energy


def owner_kernel(nz, width, layers_ref, got_ref, out_ref, energy_ref):
    blocks = got_ref.shape[0]
    parts = split(width)[0]
    k = layers_ref.shape[0]
    sd = widen(layers_ref, width)
    carries, energy = scan_slabs(sd, nz, got_ref, parts)
    deeper = jnp.zeros(sd.shape, f32)
    for n in reversed(range(blocks)):
        above = sd < n * nz
        put_wide(out_ref, n, 0, jnp.where(above, carries[n], deeper), parts)
        put_wide(out_ref, n, k, jnp.sum(jnp.where(above, deeper, 0.0), axis=0, keepdims=True), parts)
        rows = wide(got_ref, n, 0, k, parts)
        squares = wide(got_ref, n, k + 1, 1, parts)
        deeper = deeper + carries[n] * (carries[n] * squares - rows)
    energy_ref[...] = jnp.broadcast_to(total(energy) / k, energy_ref.shape)


def gradient_kernel(
    depth_count, layers_ref, got_ref, model_ref, rate_ref, w_ref, obs_ref, noise_ref, basis_hbm,
    gradient_ref, out_ref, basis_ref, sums_ref, sems
):
    started = stream(basis_hbm, basis_ref, sems)
    blocks = got_ref.shape[0]
    nz, columns = model_ref.shape
    width = columns // blocks
    parts = split(width)[0]
    k = w_ref.shape[0]
    sd = widen(layers_ref, width)
    first = lax.axis_index("depth") * nz
    above = sd < first
    for n in range(blocks):
        lanes = slice(n * width, (n + 1) * width)
        model = model_ref[:, lanes]
        coef = rate_ref[:, lanes] * (1.0 / depth_count) * jnp.exp(0.5 * model)
        decay = jnp.exp(-coef)
        w = w_ref[:, lanes]
        entering = wide(got_ref, n, 0, k, parts)
        f = jnp.where(above, entering, 0.0)
        products = []
        for z in range(nz):
            f = decay[z : z + 1] * f + jnp.where(sd == first + z, w, 0.0)
            products.append(f * (f - obs_ref[z, :, lanes]))
        deeper = jnp.where(above, 0.0, entering)
        below_sum = wide(got_ref, n, k, 1, parts)
        for z in reversed(range(nz)):
            deeper = deeper + products[z]
            data = jnp.sum(jnp.where(sd < first + z, deeper, 0.0), axis=0, keepdims=True) + below_sum
            gradient_ref[z : z + 1, lanes] = model[z : z + 1] - coef[z : z + 1] / k * data
    tiles = sums_ref.shape[0] // 2
    vectors = jnp.concatenate([gradient_ref[...], noise_ref[...]], axis=0).astype(jnp.bfloat16)
    every = jnp.zeros((2 * nz, basis_ref.shape[0]), f32)
    for at, copy in started:
        copy.wait()
        every = every + project(vectors[:, at], basis_ref[:, at])
    own_layer(every, sums_ref)
    p = group_sums(sums_ref[0:tiles, :], nz)
    q = group_sums(sums_ref[tiles : 2 * tiles, :], nz)
    lane = lax.broadcasted_iota(jnp.int32, p.shape, 1)
    both = jnp.where(lane % nz == nz - 1, p, pltpu.roll(q, LANES - nz // 2, 1))
    for n in range(blocks):
        out_ref[n] = both


def proposal_kernel(
    depth_count, width, layers_ref, got_ref, bends_ref, gradient_ref, model_ref, rate_ref, w_ref,
    obs_ref, noise_ref, basis_ref, proposal_ref, out_ref, energy_ref
):
    blocks = out_ref.shape[0]
    parts = split(width)[0]
    nz, columns = model_ref.shape
    k = w_ref.shape[0]
    projected = got_ref[0]
    for n in range(1, blocks):
        projected = projected + got_ref[n]
    p = spread(projected, nz)
    q = spread(pltpu.roll(projected, nz // 2, 1), nz)
    curvature = bends_ref[...]
    damping = curvature / (1.0 + curvature)
    shrink = 1.0 - 1.0 / jnp.sqrt(1.0 + curvature)
    mix = (damping * p - shrink * q).astype(jnp.bfloat16).astype(f32)
    layer = lax.broadcasted_iota(jnp.int32, (nz, LANES), 0)
    lane = lax.broadcasted_iota(jnp.int32, (nz, LANES), 1)
    weights = jnp.concatenate(
        [jnp.where(layer == lane % nz, mix[i : i + 1, :], 0.0) for i in range(mix.shape[0])], axis=1
    ).astype(jnp.bfloat16)
    sd = widen(layers_ref, width)
    first = lax.axis_index("depth") * nz
    misfit = jnp.zeros(sd.shape, f32)
    square = jnp.zeros((nz, width), f32)
    for n in range(blocks):
        lanes = slice(n * width, (n + 1) * width)
        correction = jnp.dot(weights, basis_ref[:, lanes], preferred_element_type=f32)
        model = model_ref[:, lanes] - gradient_ref[:, lanes] + noise_ref[:, lanes] + correction
        proposal_ref[:, lanes] = model
        coef = rate_ref[:, lanes] * (1.0 / depth_count) * jnp.exp(0.5 * model)
        rows, through, squares, part = summarize(coef, w_ref[:, lanes], sd, first, obs_ref, lanes)
        write_summary(out_ref, n, rows, through, squares, parts)
        misfit = misfit + part
        square = square + model * model
    energy_ref[...] = jnp.broadcast_to(total(misfit) / k + 0.5 * total(square), energy_ref.shape)


def energy_kernel(nz, width, layers_ref, got_ref, first_ref, owner_ref, next_ref, out_ref):
    blocks = got_ref.shape[0]
    k = layers_ref.shape[0]
    sd = widen(layers_ref, width)
    _, energy = scan_slabs(sd, nz, got_ref, split(width)[0])
    drop = first_ref[...] + owner_ref[...] - next_ref[...] - total(energy) / k
    for n in range(blocks):
        out_ref[n] = drop


def final_kernel(cells, got_ref, out_ref):
    drop = got_ref[0]
    for n in range(1, got_ref.shape[0]):
        drop = drop + got_ref[n]
    out_ref[...] = drop[0:1, 0:1] / cells


def call(kernel, outs, args, hbm=(), scratch=(), flops=10**6, limit=16):
    vmem = pl.BlockSpec(memory_space=pltpu.VMEM)
    far = pl.BlockSpec(memory_space=pltpu.HBM)
    args = [pltpu.with_memory_space_constraint(x, pltpu.HBM) if i in hbm else x for i, x in enumerate(args)]
    return pl.pallas_call(
        kernel,
        out_shape=outs,
        in_specs=[far if i in hbm else vmem for i in range(len(args))],
        out_specs=[vmem] * len(outs),
        scratch_shapes=scratch,
        compiler_params=pltpu.CompilerParams(vmem_limit_bytes=limit * 2**20),
        cost_estimate=pl.CostEstimate(flops=flops, bytes_accessed=flops, transcendentals=0),
    )(*args)


def local(model_field, column_rate, wavelets, source_depth, observed, basis, curvature, noise_draw):
    slabs = lax.axis_size("depth")
    nz, columns = model_field.shape
    sources = wavelets.shape[0]
    rank = basis.shape[0]
    depth_count = nz * slabs
    width = columns // slabs
    parts, lanes = split(width)
    struct = jax.ShapeDtypeStruct
    summary = struct((slabs, pad_rows(parts * (sources + 2)), lanes), f32)
    answer = struct((slabs, pad_rows(parts * (sources + 1)), lanes), f32)
    scalar = struct((8, LANES), f32)
    field = struct((nz, columns), f32)
    dma = pltpu.SemaphoreType.DMA
    flat = basis.reshape(rank * nz, columns)
    sums = (rank * nz // LANES, LANES)

    def exchange(x):
        return lax.all_to_all(x, "depth", 0, 0)

    sent, energy_first, layers, model, rate, w, obs, noise, bends = call(
        functools.partial(first_kernel, depth_count, slabs),
        [summary, scalar, struct((sources, LANES), jnp.int32), field, struct((1, columns), f32),
         struct(wavelets.shape, f32), struct(observed.shape, f32), field, struct(sums, f32)],
        [source_depth, model_field, column_rate.reshape(1, columns), wavelets, observed, noise_draw,
         curvature.reshape(1, rank)],
        hbm=range(7),
        scratch=[pltpu.VMEM((1, rank), f32), pltpu.SMEM((sources,), jnp.int32), dma((6,)), dma((8,))],
    )
    got = exchange(sent)
    sent, energy_owner = call(
        functools.partial(owner_kernel, nz, width), [answer, scalar], [layers, got],
    )
    got = exchange(sent)
    gradient, sent, near = call(
        functools.partial(gradient_kernel, depth_count),
        [field, struct((slabs,) + sums, f32), struct(flat.shape, flat.dtype)],
        [layers, got, model, rate, w, obs, noise, flat], hbm=(7,),
        scratch=[pltpu.VMEM((2 * sums[0], LANES), f32), dma((8,))],
    )
    got = exchange(sent)
    proposal, sent, energy_next = call(
        functools.partial(proposal_kernel, depth_count, width),
        [field, summary, scalar],
        [layers, got, bends, gradient, model, rate, w, obs, noise, near],
    )
    got = exchange(sent)
    (sent,) = call(
        functools.partial(energy_kernel, nz, width), [struct((slabs, 8, LANES), f32)],
        [layers, got, energy_first, energy_owner, energy_next],
    )
    got = exchange(sent)
    (gain,) = call(functools.partial(final_kernel, depth_count * columns), [struct((1, 1), f32)], [got])
    return (proposal, gain.reshape(1))


def solution(mesh):
    in_specs = (
        P(("chain", "depth"), None),
        P("chain"),
        P("chain", None),
        P("chain"),
        P(("chain", "depth"), None, None),
        P("chain", "depth", None),
        P("chain"),
        P(("chain", "depth"), None),
    )
    out_specs = (P(("chain", "depth"), None), P("chain"))
    return jax.shard_map(local, mesh=mesh, in_specs=in_specs, out_specs=out_specs, check_vma=False)
```

```python
import functools

import jax
import jax.numpy as jnp
from jax import lax
from jax.experimental import pallas as pl
from jax.experimental.pallas import tpu as pltpu
from jax.sharding import PartitionSpec as P

LANES = 128
f32 = jnp.float32


def pad_rows(rows):
    return -(-rows // 8) * 8


def source_layers(sd_ref, count):
    row = lax.broadcasted_iota(jnp.int32, (count, LANES), 0)
    layers = jnp.zeros((count, LANES), jnp.int32)
    for k in range(count):
        layers = jnp.where(row == k, sd_ref[k], layers)
    return layers


def widen(layers_ref, width):
    layers = layers_ref[...]
    if width % LANES == 0:
        return jnp.concatenate([layers] * (width // LANES), axis=1)
    return layers[:, :width]


def split(width):
    return (width // LANES, LANES) if width % LANES == 0 else (1, width)


def wide(ref, n, start, count, parts):
    pieces = [ref[n, parts * start + p * count : parts * start + (p + 1) * count, :] for p in range(parts)]
    return pieces[0] if parts == 1 else jnp.concatenate(pieces, axis=1)


def put_wide(ref, n, start, value, parts):
    count, lanes = value.shape[0], value.shape[1] // parts
    for p in range(parts):
        ref[n, parts * start + p * count : parts * start + (p + 1) * count, :] = value[:, p * lanes : (p + 1) * lanes]


def summarize(coef, w, sd, first, obs_ref, lanes):
    nz = coef.shape[0]
    decay = jnp.exp(-coef)
    above = sd < first
    f = jnp.where(above, 1.0, 0.0)
    through = jnp.ones((1, coef.shape[1]), f32)
    squares = jnp.zeros_like(through)
    cross = jnp.zeros_like(w)
    own = jnp.zeros_like(w)
    for z in range(nz):
        step = decay[z : z + 1]
        f = step * f + jnp.where(sd == first + z, w, 0.0)
        through = through * step
        squares = squares + through * through
        cross = cross + f * obs_ref[z, :, lanes]
        own = own + f * f
    rows = jnp.where(above, cross, f)
    part = jnp.where(above, 0.0, own - 2.0 * cross)
    return rows, through, squares, part


def total(x):
    return jnp.sum(jnp.sum(x, axis=0, keepdims=True), axis=1, keepdims=True)


def write_summary(out_ref, n, rows, through, squares, parts):
    k = rows.shape[0]
    put_wide(out_ref, n, 0, rows, parts)
    put_wide(out_ref, n, k, through, parts)
    put_wide(out_ref, n, k + 1, squares, parts)


def expand(row, nz):
    rank, share = row.shape[1], LANES // nz
    line = lax.broadcasted_iota(jnp.int32, (rank // share, rank), 0)
    entry = lax.broadcasted_iota(jnp.int32, (rank // share, rank), 1)
    mine = jnp.where(entry // share == line, jnp.broadcast_to(row, line.shape), 0.0)
    entry = lax.broadcasted_iota(jnp.int32, (rank, LANES), 0)
    lane = lax.broadcasted_iota(jnp.int32, (rank, LANES), 1)
    pick = jnp.where(entry % share == lane // nz, 1.0, 0.0)
    return jnp.dot(mine, pick, precision=lax.Precision.HIGHEST, preferred_element_type=f32)


def first_kernel(
    depth_count, blocks, sd_hbm, model_hbm, rate_hbm, w_hbm, obs_hbm, noise_hbm, curvature_hbm,
    out_ref, energy_ref, layers_ref, model_ref, rate_ref, w_ref, obs_ref, noise_ref, bends_ref,
    curvature_ref, sd_ref, sems, obs_sems
):
    nz, columns = model_ref.shape
    k = w_ref.shape[0]
    width = columns // blocks
    parts = split(width)[0]
    copies = [
        pltpu.make_async_copy(src, dst, sems.at[i])
        for i, (src, dst) in enumerate([
            (curvature_hbm, curvature_ref), (sd_hbm, sd_ref), (model_hbm, model_ref), (rate_hbm, rate_ref),
            (w_hbm, w_ref), (noise_hbm, noise_ref),
        ])
    ]
    pieces = obs_sems.shape[0]
    piece = columns // pieces
    obs_copies = []
    for i in range(pieces):
        at = pl.ds(i * piece, piece)
        obs_copies.append(pltpu.make_async_copy(obs_hbm.at[:, :, at], obs_ref.at[:, :, at], obs_sems.at[i]))
    for copy in copies[:5]:
        copy.start()
    for copy in obs_copies:
        copy.start()
    copies[5].start()
    copies[0].wait()
    bends_ref[...] = expand(curvature_ref[...], nz)
    for copy in copies[1:5]:
        copy.wait()
    layers_ref[...] = source_layers(sd_ref, k)
    sd = widen(layers_ref, width)
    first = lax.axis_index("depth") * nz
    for copy in obs_copies:
        copy.wait()
    misfit = jnp.zeros(sd.shape, f32)
    square = jnp.zeros((nz, width), f32)
    for n in range(blocks):
        lanes = slice(n * width, (n + 1) * width)
        model = model_ref[:, lanes]
        coef = rate_ref[:, lanes] * (1.0 / depth_count) * jnp.exp(0.5 * model)
        rows, through, squares, part = summarize(coef, w_ref[:, lanes], sd, first, obs_ref, lanes)
        write_summary(out_ref, n, rows, through, squares, parts)
        misfit = misfit + part
        square = square + model * model
    energy_ref[...] = jnp.broadcast_to(total(misfit) / k + 0.5 * total(square), energy_ref.shape)
    copies[5].wait()


def group_sums(x, nz):
    step = 1
    while step < nz:
        x = x + pltpu.roll(x, step, 1)
        step *= 2
    return x


def spread(x, nz):
    lane = lax.broadcasted_iota(jnp.int32, x.shape, 1)
    x = jnp.where(lane % nz == nz - 1, x, 0.0)
    step = 1
    while step < nz:
        x = x + pltpu.roll(x, LANES - step, 1)
        step *= 2
    return x


def project(vectors, basis_ref):
    return lax.dot_general(vectors, basis_ref, (((1,), (1,)), ((), ())), preferred_element_type=f32)


def own_layer(every, sums_ref):
    nz = every.shape[0] // 2
    tiles = every.shape[1] // LANES
    layer = lax.broadcasted_iota(jnp.int32, (nz, LANES), 0)
    lane = lax.broadcasted_iota(jnp.int32, (nz, LANES), 1)
    own = layer == lane % nz
    for which in range(2):
        for t in range(tiles):
            mine = jnp.where(own, every[which * nz : (which + 1) * nz, t * LANES : (t + 1) * LANES], 0.0)
            at = which * tiles + t
            sums_ref[at : at + 1, :] = jnp.sum(mine, axis=0, keepdims=True)


def stream(basis_hbm, basis_ref, sems):
    pieces = sems.shape[0]
    piece = basis_ref.shape[1] // pieces
    started = []
    for i in range(pieces):
        at = pl.ds(i * piece, piece)
        copy = pltpu.make_async_copy(basis_hbm.at[:, at], basis_ref.at[:, at], sems.at[i])
        copy.start()
        started.append((slice(i * piece, (i + 1) * piece), copy))
    return started


def scan_slabs(sd, nz, got_ref, parts):
    blocks = got_ref.shape[0]
    k = sd.shape[0]
    carry = jnp.zeros(sd.shape, f32)
    energy = jnp.zeros(sd.shape, f32)
    carries = []
    for n in range(blocks):
        rows = wide(got_ref, n, 0, k, parts)
        through = wide(got_ref, n, k, 1, parts)
        squares = wide(got_ref, n, k + 1, 1, parts)
        carries.append(carry)
        energy = energy + carry * (carry * squares - 2.0 * rows)
        carry = through * carry + jnp.where(sd >= n * nz, rows, 0.0)
    return carries, energy


def owner_kernel(nz, width, layers_ref, got_ref, out_ref, energy_ref):
    blocks = got_ref.shape[0]
    parts = split(width)[0]
    k = layers_ref.shape[0]
    sd = widen(layers_ref, width)
    carries, energy = scan_slabs(sd, nz, got_ref, parts)
    deeper = jnp.zeros(sd.shape, f32)
    for n in reversed(range(blocks)):
        above = sd < n * nz
        put_wide(out_ref, n, 0, jnp.where(above, carries[n], deeper), parts)
        put_wide(out_ref, n, k, jnp.sum(jnp.where(above, deeper, 0.0), axis=0, keepdims=True), parts)
        rows = wide(got_ref, n, 0, k, parts)
        squares = wide(got_ref, n, k + 1, 1, parts)
        deeper = deeper + carries[n] * (carries[n] * squares - rows)
    energy_ref[...] = jnp.broadcast_to(total(energy) / k, energy_ref.shape)


def gradient_kernel(
    depth_count, layers_ref, got_ref, model_ref, rate_ref, w_ref, obs_ref, noise_ref, basis_ref,
    gradient_ref, out_ref, sums_ref
):
    blocks = got_ref.shape[0]
    nz, columns = model_ref.shape
    width = columns // blocks
    parts = split(width)[0]
    k = w_ref.shape[0]
    sd = widen(layers_ref, width)
    first = lax.axis_index("depth") * nz
    above = sd < first
    tiles = sums_ref.shape[0] // 2
    piece = max(width, min(columns, 2 * LANES))
    every = jnp.zeros((2 * nz, basis_ref.shape[0]), f32)

    def add_projection(every, at):
        vectors = jnp.concatenate([gradient_ref[:, at], noise_ref[:, at]], axis=0).astype(jnp.bfloat16)
        return every + project(vectors, basis_ref[:, at])

    for n in range(blocks):
        lanes = slice(n * width, (n + 1) * width)
        if n > 0 and lanes.start % piece == 0:
            every = add_projection(every, slice(lanes.start - piece, lanes.start))
        model = model_ref[:, lanes]
        coef = rate_ref[:, lanes] * (1.0 / depth_count) * jnp.exp(0.5 * model)
        decay = jnp.exp(-coef)
        w = w_ref[:, lanes]
        entering = wide(got_ref, n, 0, k, parts)
        f = jnp.where(above, entering, 0.0)
        products = []
        for z in range(nz):
            f = decay[z : z + 1] * f + jnp.where(sd == first + z, w, 0.0)
            products.append(f * (f - obs_ref[z, :, lanes]))
        deeper = jnp.where(above, 0.0, entering)
        below_sum = wide(got_ref, n, k, 1, parts)
        for z in reversed(range(nz)):
            deeper = deeper + products[z]
            data = jnp.sum(jnp.where(sd < first + z, deeper, 0.0), axis=0, keepdims=True) + below_sum
            gradient_ref[z : z + 1, lanes] = model[z : z + 1] - coef[z : z + 1] / k * data
    every = add_projection(every, slice(columns - piece, columns))
    own_layer(every, sums_ref)
    p = group_sums(sums_ref[0:tiles, :], nz)
    q = group_sums(sums_ref[tiles : 2 * tiles, :], nz)
    lane = lax.broadcasted_iota(jnp.int32, p.shape, 1)
    both = jnp.where(lane % nz == nz - 1, p, pltpu.roll(q, LANES - nz // 2, 1))
    for n in range(blocks):
        out_ref[n] = both


def proposal_kernel(
    depth_count, width, layers_ref, got_ref, bends_ref, gradient_ref, model_ref, rate_ref, w_ref,
    obs_ref, noise_ref, basis_ref, proposal_ref, out_ref, energy_ref
):
    blocks = out_ref.shape[0]
    parts = split(width)[0]
    nz, columns = model_ref.shape
    k = w_ref.shape[0]
    projected = got_ref[0]
    for n in range(1, blocks):
        projected = projected + got_ref[n]
    p = spread(projected, nz)
    q = spread(pltpu.roll(projected, nz // 2, 1), nz)
    curvature = bends_ref[...]
    damping = curvature / (1.0 + curvature)
    shrink = 1.0 - 1.0 / jnp.sqrt(1.0 + curvature)
    mix = (damping * p - shrink * q).astype(jnp.bfloat16).astype(f32)
    layer = lax.broadcasted_iota(jnp.int32, (nz, LANES), 0)
    lane = lax.broadcasted_iota(jnp.int32, (nz, LANES), 1)
    weights = jnp.concatenate(
        [jnp.where(layer == lane % nz, mix[i : i + 1, :], 0.0) for i in range(mix.shape[0])], axis=1
    ).astype(jnp.bfloat16)

    def correct(n):
        return jnp.dot(weights, basis_ref[:, n * width : (n + 1) * width], preferred_element_type=f32)

    corrections = [correct(0)]
    sd = widen(layers_ref, width)
    first = lax.axis_index("depth") * nz
    misfit = jnp.zeros(sd.shape, f32)
    square = jnp.zeros((nz, width), f32)
    for n in range(blocks):
        lanes = slice(n * width, (n + 1) * width)
        correction = corrections.pop()
        if n + 1 < blocks:
            corrections.append(correct(n + 1))
        model = model_ref[:, lanes] - gradient_ref[:, lanes] + noise_ref[:, lanes] + correction
        proposal_ref[:, lanes] = model
        coef = rate_ref[:, lanes] * (1.0 / depth_count) * jnp.exp(0.5 * model)
        rows, through, squares, part = summarize(coef, w_ref[:, lanes], sd, first, obs_ref, lanes)
        write_summary(out_ref, n, rows, through, squares, parts)
        misfit = misfit + part
        square = square + model * model
    energy_ref[...] = jnp.broadcast_to(total(misfit) / k + 0.5 * total(square), energy_ref.shape)


def energy_kernel(nz, width, layers_ref, got_ref, first_ref, owner_ref, next_ref, out_ref):
    blocks = got_ref.shape[0]
    k = layers_ref.shape[0]
    sd = widen(layers_ref, width)
    _, energy = scan_slabs(sd, nz, got_ref, split(width)[0])
    drop = first_ref[...] + owner_ref[...] - next_ref[...] - total(energy) / k
    for n in range(blocks):
        out_ref[n] = drop


def final_kernel(cells, got_ref, out_ref):
    drop = got_ref[0]
    for n in range(1, got_ref.shape[0]):
        drop = drop + got_ref[n]
    out_ref[...] = drop[0:1, 0:1] / cells


def call(kernel, outs, args, hbm=(), scratch=(), flops=10**6, limit=16):
    vmem = pl.BlockSpec(memory_space=pltpu.VMEM)
    far = pl.BlockSpec(memory_space=pltpu.HBM)
    args = [pltpu.with_memory_space_constraint(x, pltpu.HBM) if i in hbm else x for i, x in enumerate(args)]
    return pl.pallas_call(
        kernel,
        out_shape=outs,
        in_specs=[far if i in hbm else vmem for i in range(len(args))],
        out_specs=[vmem] * len(outs),
        scratch_shapes=scratch,
        compiler_params=pltpu.CompilerParams(vmem_limit_bytes=limit * 2**20),
        cost_estimate=pl.CostEstimate(flops=flops, bytes_accessed=flops, transcendentals=0),
    )(*args)


def local(model_field, column_rate, wavelets, source_depth, observed, basis, curvature, noise_draw):
    slabs = lax.axis_size("depth")
    nz, columns = model_field.shape
    sources = wavelets.shape[0]
    rank = basis.shape[0]
    depth_count = nz * slabs
    width = columns // slabs
    parts, lanes = split(width)
    struct = jax.ShapeDtypeStruct
    summary = struct((slabs, pad_rows(parts * (sources + 2)), lanes), f32)
    answer = struct((slabs, pad_rows(parts * (sources + 1)), lanes), f32)
    scalar = struct((8, LANES), f32)
    field = struct((nz, columns), f32)
    dma = pltpu.SemaphoreType.DMA
    flat = basis.reshape(rank * nz, columns)
    sums = (rank * nz // LANES, LANES)

    def exchange(x):
        return lax.all_to_all(x, "depth", 0, 0)

    sent, energy_first, layers, model, rate, w, obs, noise, bends = call(
        functools.partial(first_kernel, depth_count, slabs),
        [summary, scalar, struct((sources, LANES), jnp.int32), field, struct((1, columns), f32),
         struct(wavelets.shape, f32), struct(observed.shape, f32), field, struct(sums, f32)],
        [source_depth, model_field, column_rate.reshape(1, columns), wavelets, observed, noise_draw,
         curvature.reshape(1, rank)],
        hbm=range(7),
        scratch=[pltpu.VMEM((1, rank), f32), pltpu.SMEM((sources,), jnp.int32), dma((6,)), dma((8,))],
    )
    got = exchange(sent)
    sent, energy_owner = call(
        functools.partial(owner_kernel, nz, width), [answer, scalar], [layers, got], flops=10**10,
    )
    got = exchange(sent)
    gradient, sent = call(
        functools.partial(gradient_kernel, depth_count),
        [field, struct((slabs,) + sums, f32)],
        [layers, got, model, rate, w, obs, noise, flat],
        scratch=[pltpu.VMEM((2 * sums[0], LANES), f32)],
    )
    got = exchange(sent)
    proposal, sent, energy_next = call(
        functools.partial(proposal_kernel, depth_count, width),
        [field, summary, scalar],
        [layers, got, bends, gradient, model, rate, w, obs, noise, flat],
    )
    got = exchange(sent)
    (sent,) = call(
        functools.partial(energy_kernel, nz, width), [struct((slabs, 8, LANES), f32)],
        [layers, got, energy_first, energy_owner, energy_next],
    )
    got = exchange(sent)
    (gain,) = call(functools.partial(final_kernel, depth_count * columns), [struct((1, 1), f32)], [got])
    return (proposal, gain.reshape(1))


def solution(mesh):
    in_specs = (
        P(("chain", "depth"), None),
        P("chain"),
        P("chain", None),
        P("chain"),
        P(("chain", "depth"), None, None),
        P("chain", "depth", None),
        P("chain"),
        P(("chain", "depth"), None),
    )
    out_specs = (P(("chain", "depth"), None), P("chain"))
    return jax.shard_map(local, mesh=mesh, in_specs=in_specs, out_specs=out_specs, check_vma=False)
```

```python
import functools

import jax
import jax.numpy as jnp
from jax import lax
from jax.experimental import pallas as pl
from jax.experimental.pallas import tpu as pltpu
from jax.sharding import PartitionSpec as P

LANES = 128
f32 = jnp.float32


def pad_rows(rows):
    return -(-rows // 8) * 8


def source_layers(sd_ref, count):
    row = lax.broadcasted_iota(jnp.int32, (count, LANES), 0)
    layers = jnp.zeros((count, LANES), jnp.int32)
    for k in range(count):
        layers = jnp.where(row == k, sd_ref[k], layers)
    return layers


def widen(layers_ref, width):
    layers = layers_ref[...]
    if width % LANES == 0:
        return jnp.concatenate([layers] * (width // LANES), axis=1)
    return layers[:, :width]


def split(width):
    return (width // LANES, LANES) if width % LANES == 0 else (1, width)


def wide(ref, n, start, count, parts):
    pieces = [ref[n, parts * start + p * count : parts * start + (p + 1) * count, :] for p in range(parts)]
    return pieces[0] if parts == 1 else jnp.concatenate(pieces, axis=1)


def put_wide(ref, n, start, value, parts):
    count, lanes = value.shape[0], value.shape[1] // parts
    for p in range(parts):
        ref[n, parts * start + p * count : parts * start + (p + 1) * count, :] = value[:, p * lanes : (p + 1) * lanes]


def summarize(coef, w, sd, first, obs_ref, lanes):
    nz = coef.shape[0]
    decay = jnp.exp(-coef)
    above = sd < first
    f = jnp.where(above, 1.0, 0.0)
    through = jnp.ones((1, coef.shape[1]), f32)
    squares = jnp.zeros_like(through)
    cross = jnp.zeros_like(w)
    own = jnp.zeros_like(w)
    for z in range(nz):
        step = decay[z : z + 1]
        f = step * f + jnp.where(sd == first + z, w, 0.0)
        through = through * step
        squares = squares + through * through
        cross = cross + f * obs_ref[z, :, lanes]
        own = own + f * f
    rows = jnp.where(above, cross, f)
    part = jnp.where(above, 0.0, own - 2.0 * cross)
    return rows, through, squares, part


def total(x):
    return jnp.sum(jnp.sum(x, axis=0, keepdims=True), axis=1, keepdims=True)


def write_summary(out_ref, n, rows, through, squares, parts):
    k = rows.shape[0]
    put_wide(out_ref, n, 0, rows, parts)
    put_wide(out_ref, n, k, through, parts)
    put_wide(out_ref, n, k + 1, squares, parts)


def expand(row, nz):
    rank, share = row.shape[1], LANES // nz
    line = lax.broadcasted_iota(jnp.int32, (rank // share, rank), 0)
    entry = lax.broadcasted_iota(jnp.int32, (rank // share, rank), 1)
    mine = jnp.where(entry // share == line, jnp.broadcast_to(row, line.shape), 0.0)
    entry = lax.broadcasted_iota(jnp.int32, (rank, LANES), 0)
    lane = lax.broadcasted_iota(jnp.int32, (rank, LANES), 1)
    pick = jnp.where(entry % share == lane // nz, 1.0, 0.0)
    return jnp.dot(mine, pick, precision=lax.Precision.HIGHEST, preferred_element_type=f32)


def first_kernel(
    depth_count, blocks, sd_hbm, model_hbm, rate_hbm, w_hbm, obs_hbm, noise_hbm, curvature_hbm,
    out_ref, energy_ref, layers_ref, model_ref, rate_ref, w_ref, obs_ref, noise_ref, bends_ref,
    curvature_ref, sd_ref, sems, obs_sems
):
    nz, columns = model_ref.shape
    k = w_ref.shape[0]
    width = columns // blocks
    parts = split(width)[0]
    copies = [
        pltpu.make_async_copy(src, dst, sems.at[i])
        for i, (src, dst) in enumerate([
            (curvature_hbm, curvature_ref), (sd_hbm, sd_ref), (model_hbm, model_ref), (rate_hbm, rate_ref),
            (w_hbm, w_ref), (noise_hbm, noise_ref),
        ])
    ]
    pieces = obs_sems.shape[0]
    piece = columns // pieces
    obs_copies = []
    for i in range(pieces):
        at = pl.ds(i * piece, piece)
        obs_copies.append(pltpu.make_async_copy(obs_hbm.at[:, :, at], obs_ref.at[:, :, at], obs_sems.at[i]))
    for copy in copies[:5]:
        copy.start()
    for copy in obs_copies:
        copy.start()
    copies[5].start()
    copies[0].wait()
    bends_ref[...] = expand(curvature_ref[...], nz)
    for copy in copies[1:5]:
        copy.wait()
    layers_ref[...] = source_layers(sd_ref, k)
    sd = widen(layers_ref, width)
    first = lax.axis_index("depth") * nz
    for copy in obs_copies:
        copy.wait()
    misfit = jnp.zeros(sd.shape, f32)
    square = jnp.zeros((nz, width), f32)
    for n in range(blocks):
        lanes = slice(n * width, (n + 1) * width)
        model = model_ref[:, lanes]
        coef = rate_ref[:, lanes] * (1.0 / depth_count) * jnp.exp(0.5 * model)
        rows, through, squares, part = summarize(coef, w_ref[:, lanes], sd, first, obs_ref, lanes)
        write_summary(out_ref, n, rows, through, squares, parts)
        misfit = misfit + part
        square = square + model * model
    energy_ref[...] = jnp.broadcast_to(total(misfit) / k + 0.5 * total(square), energy_ref.shape)
    copies[5].wait()


def group_sums(x, nz):
    step = 1
    while step < nz:
        x = x + pltpu.roll(x, step, 1)
        step *= 2
    return x


def spread(x, nz):
    lane = lax.broadcasted_iota(jnp.int32, x.shape, 1)
    x = jnp.where(lane % nz == nz - 1, x, 0.0)
    step = 1
    while step < nz:
        x = x + pltpu.roll(x, LANES - step, 1)
        step *= 2
    return x


def project(vectors, basis_ref):
    return lax.dot_general(vectors, basis_ref, (((1,), (1,)), ((), ())), preferred_element_type=f32)


def own_layer(every, sums_ref):
    nz = every.shape[0] // 2
    tiles = every.shape[1] // LANES
    layer = lax.broadcasted_iota(jnp.int32, (nz, LANES), 0)
    lane = lax.broadcasted_iota(jnp.int32, (nz, LANES), 1)
    own = layer == lane % nz
    for which in range(2):
        for t in range(tiles):
            mine = jnp.where(own, every[which * nz : (which + 1) * nz, t * LANES : (t + 1) * LANES], 0.0)
            at = which * tiles + t
            sums_ref[at : at + 1, :] = jnp.sum(mine, axis=0, keepdims=True)


def stream(basis_hbm, basis_ref, sems):
    pieces = sems.shape[0]
    piece = basis_ref.shape[1] // pieces
    started = []
    for i in range(pieces):
        at = pl.ds(i * piece, piece)
        copy = pltpu.make_async_copy(basis_hbm.at[:, at], basis_ref.at[:, at], sems.at[i])
        copy.start()
        started.append((slice(i * piece, (i + 1) * piece), copy))
    return started


def scan_slabs(sd, nz, got_ref, parts):
    blocks = got_ref.shape[0]
    k = sd.shape[0]
    carry = jnp.zeros(sd.shape, f32)
    energy = jnp.zeros(sd.shape, f32)
    carries = []
    for n in range(blocks):
        rows = wide(got_ref, n, 0, k, parts)
        through = wide(got_ref, n, k, 1, parts)
        squares = wide(got_ref, n, k + 1, 1, parts)
        carries.append(carry)
        energy = energy + carry * (carry * squares - 2.0 * rows)
        carry = through * carry + jnp.where(sd >= n * nz, rows, 0.0)
    return carries, energy


def owner_kernel(nz, width, layers_ref, got_ref, out_ref, energy_ref):
    blocks = got_ref.shape[0]
    parts = split(width)[0]
    k = layers_ref.shape[0]
    sd = widen(layers_ref, width)
    carries, energy = scan_slabs(sd, nz, got_ref, parts)
    deeper = jnp.zeros(sd.shape, f32)
    for n in reversed(range(blocks)):
        above = sd < n * nz
        put_wide(out_ref, n, 0, jnp.where(above, carries[n], deeper), parts)
        put_wide(out_ref, n, k, jnp.sum(jnp.where(above, deeper, 0.0), axis=0, keepdims=True), parts)
        rows = wide(got_ref, n, 0, k, parts)
        squares = wide(got_ref, n, k + 1, 1, parts)
        deeper = deeper + carries[n] * (carries[n] * squares - rows)
    energy_ref[...] = jnp.broadcast_to(total(energy) / k, energy_ref.shape)


def gradient_kernel(
    depth_count, layers_ref, got_ref, model_ref, rate_ref, w_ref, obs_ref, noise_ref, basis_ref,
    gradient_ref, out_ref, sums_ref
):
    blocks = got_ref.shape[0]
    nz, columns = model_ref.shape
    width = columns // blocks
    parts = split(width)[0]
    k = w_ref.shape[0]
    sd = widen(layers_ref, width)
    first = lax.axis_index("depth") * nz
    above = sd < first
    tiles = sums_ref.shape[0] // 2
    piece = max(width, min(columns, 2 * LANES))
    every = jnp.zeros((2 * nz, basis_ref.shape[0]), f32)

    def add_projection(every, at):
        vectors = jnp.concatenate([gradient_ref[:, at], noise_ref[:, at]], axis=0).astype(jnp.bfloat16)
        return every + project(vectors, basis_ref[:, at])

    for n in range(blocks):
        lanes = slice(n * width, (n + 1) * width)
        if n > 0 and lanes.start % piece == 0:
            every = add_projection(every, slice(lanes.start - piece, lanes.start))
        model = model_ref[:, lanes]
        coef = rate_ref[:, lanes] * (1.0 / depth_count) * jnp.exp(0.5 * model)
        decay = jnp.exp(-coef)
        w = w_ref[:, lanes]
        entering = wide(got_ref, n, 0, k, parts)
        f = jnp.where(above, entering, 0.0)
        products = []
        for z in range(nz):
            f = decay[z : z + 1] * f + jnp.where(sd == first + z, w, 0.0)
            products.append(f * (f - obs_ref[z, :, lanes]))
        deeper = jnp.where(above, 0.0, entering)
        below_sum = wide(got_ref, n, k, 1, parts)
        for z in reversed(range(nz)):
            deeper = deeper + products[z]
            data = jnp.sum(jnp.where(sd < first + z, deeper, 0.0), axis=0, keepdims=True) + below_sum
            gradient_ref[z : z + 1, lanes] = model[z : z + 1] - coef[z : z + 1] / k * data
    every = add_projection(every, slice(columns - piece, columns))
    own_layer(every, sums_ref)
    p = group_sums(sums_ref[0:tiles, :], nz)
    q = group_sums(sums_ref[tiles : 2 * tiles, :], nz)
    lane = lax.broadcasted_iota(jnp.int32, p.shape, 1)
    both = jnp.where(lane % nz == nz - 1, p, pltpu.roll(q, LANES - nz // 2, 1))
    for n in range(blocks):
        out_ref[n] = both


def proposal_kernel(
    depth_count, width, layers_ref, got_ref, bends_ref, gradient_ref, model_ref, rate_ref, w_ref,
    obs_ref, noise_ref, basis_ref, proposal_ref, out_ref, energy_ref
):
    blocks = out_ref.shape[0]
    parts = split(width)[0]
    nz, columns = model_ref.shape
    k = w_ref.shape[0]
    projected = got_ref[0]
    for n in range(1, blocks):
        projected = projected + got_ref[n]
    p = spread(projected, nz)
    q = spread(pltpu.roll(projected, nz // 2, 1), nz)
    curvature = bends_ref[...]
    damping = curvature / (1.0 + curvature)
    shrink = 1.0 - 1.0 / jnp.sqrt(1.0 + curvature)
    mix = (damping * p - shrink * q).astype(jnp.bfloat16).astype(f32)
    layer = lax.broadcasted_iota(jnp.int32, (nz, LANES), 0)
    lane = lax.broadcasted_iota(jnp.int32, (nz, LANES), 1)
    weights = jnp.concatenate(
        [jnp.where(layer == lane % nz, mix[i : i + 1, :], 0.0) for i in range(mix.shape[0])], axis=1
    ).astype(jnp.bfloat16)

    def correct(n):
        return jnp.dot(weights, basis_ref[:, n * width : (n + 1) * width], preferred_element_type=f32)

    corrections = [correct(0)]
    sd = widen(layers_ref, width)
    first = lax.axis_index("depth") * nz
    misfit = jnp.zeros(sd.shape, f32)
    square = jnp.zeros((nz, width), f32)
    for n in range(blocks):
        lanes = slice(n * width, (n + 1) * width)
        correction = corrections.pop()
        if n + 1 < blocks:
            corrections.append(correct(n + 1))
        model = model_ref[:, lanes] - gradient_ref[:, lanes] + noise_ref[:, lanes] + correction
        proposal_ref[:, lanes] = model
        coef = rate_ref[:, lanes] * (1.0 / depth_count) * jnp.exp(0.5 * model)
        rows, through, squares, part = summarize(coef, w_ref[:, lanes], sd, first, obs_ref, lanes)
        write_summary(out_ref, n, rows, through, squares, parts)
        misfit = misfit + part
        square = square + model * model
    energy_ref[...] = jnp.broadcast_to(total(misfit) / k + 0.5 * total(square), energy_ref.shape)


def energy_kernel(nz, width, layers_ref, got_ref, first_ref, owner_ref, next_ref, out_ref):
    blocks = got_ref.shape[0]
    k = layers_ref.shape[0]
    sd = widen(layers_ref, width)
    _, energy = scan_slabs(sd, nz, got_ref, split(width)[0])
    drop = first_ref[...] + owner_ref[...] - next_ref[...] - total(energy) / k
    for n in range(blocks):
        out_ref[n] = drop[0:1, :]


def final_kernel(cells, got_ref, proposal_in, out_ref, proposal_ref):
    proposal_ref[...] = proposal_in[...]
    drop = got_ref[0]
    for n in range(1, got_ref.shape[0]):
        drop = drop + got_ref[n]
    out_ref[...] = drop[:, 0:1] / cells


def call(kernel, outs, args, hbm=(), scratch=(), flops=10**6, limit=16):
    vmem = pl.BlockSpec(memory_space=pltpu.VMEM)
    far = pl.BlockSpec(memory_space=pltpu.HBM)
    args = [pltpu.with_memory_space_constraint(x, pltpu.HBM) if i in hbm else x for i, x in enumerate(args)]
    return pl.pallas_call(
        kernel,
        out_shape=outs,
        in_specs=[far if i in hbm else vmem for i in range(len(args))],
        out_specs=[vmem] * len(outs),
        scratch_shapes=scratch,
        compiler_params=pltpu.CompilerParams(vmem_limit_bytes=limit * 2**20),
        cost_estimate=pl.CostEstimate(flops=flops, bytes_accessed=flops, transcendentals=0),
    )(*args)


def local(model_field, column_rate, wavelets, source_depth, observed, basis, curvature, noise_draw):
    slabs = lax.axis_size("depth")
    nz, columns = model_field.shape
    sources = wavelets.shape[0]
    rank = basis.shape[0]
    depth_count = nz * slabs
    width = columns // slabs
    parts, lanes = split(width)
    struct = jax.ShapeDtypeStruct
    summary = struct((slabs, pad_rows(parts * (sources + 2)), lanes), f32)
    answer = struct((slabs, pad_rows(parts * (sources + 1)), lanes), f32)
    scalar = struct((8, LANES), f32)
    field = struct((nz, columns), f32)
    dma = pltpu.SemaphoreType.DMA
    flat = basis.reshape(rank * nz, columns)
    sums = (rank * nz // LANES, LANES)

    def exchange(x):
        return lax.all_to_all(x, "depth", 0, 0)

    sent, energy_first, layers, model, rate, w, obs, noise, bends = call(
        functools.partial(first_kernel, depth_count, slabs),
        [summary, scalar, struct((sources, LANES), jnp.int32), field, struct((1, columns), f32),
         struct(wavelets.shape, f32), struct(observed.shape, f32), field, struct(sums, f32)],
        [source_depth, model_field, column_rate.reshape(1, columns), wavelets, observed, noise_draw,
         curvature.reshape(1, rank)],
        hbm=range(7),
        scratch=[pltpu.VMEM((1, rank), f32), pltpu.SMEM((sources,), jnp.int32), dma((6,)), dma((1,))],
    )
    got = exchange(sent)
    sent, energy_owner = call(
        functools.partial(owner_kernel, nz, width), [answer, scalar], [layers, got], flops=10**11,
    )
    got = exchange(sent)
    gradient, sent = call(
        functools.partial(gradient_kernel, depth_count),
        [field, struct((slabs,) + sums, f32)],
        [layers, got, model, rate, w, obs, noise, flat],
        scratch=[pltpu.VMEM((2 * sums[0], LANES), f32)],
    )
    got = exchange(sent)
    proposal, sent, energy_next = call(
        functools.partial(proposal_kernel, depth_count, width),
        [field, summary, scalar],
        [layers, got, bends, gradient, model, rate, w, obs, noise, flat],
    )
    got = exchange(sent)
    (sent,) = call(
        functools.partial(energy_kernel, nz, width), [struct((slabs, 1, LANES), f32)],
        [layers, got, energy_first, energy_owner, energy_next],
    )
    got = exchange(sent)
    gain, proposal = call(
        functools.partial(final_kernel, depth_count * columns), [struct((1, 1), f32), field], [got, proposal]
    )
    return (proposal, gain.reshape(1))


def solution(mesh):
    in_specs = (
        P(("chain", "depth"), None),
        P("chain"),
        P("chain", None),
        P("chain"),
        P(("chain", "depth"), None, None),
        P("chain", "depth", None),
        P("chain"),
        P(("chain", "depth"), None),
    )
    out_specs = (P(("chain", "depth"), None), P("chain"))
    return jax.shard_map(local, mesh=mesh, in_specs=in_specs, out_specs=out_specs, check_vma=False)
```
